32 devices in a mesh: path: 16 (over z, x, core), shard: 2 (over y).
Axes of the slice: x: 2, y: 2, z: 4, core: 2. Of those that a mesh axis runs over, the one named last changes fastest.
Arguments:
- deltas: bfloat16 [16, 32, 4096], P('path', 'shard'), may hold values from -96 to 96
- momentum: float32 [16, 32, 4096], P(None, 'shard', 'path'), may hold values from -4 to 4
- path_module: int32 [16], replicated, may hold values from 0 to 15, as said below
Outputs:
- path_update: bfloat16 [16, 32, 4096], P('path', 'shard')
- new_momentum: float32 [16, 32, 4096], P(None, 'shard', 'path')
The draws below stay inside these ranges and needn't reach their ends.
Inputs may be any that keep to these rules, and one draw needn't show every extreme that they name: `path_module`: every module is used by at least one and at most seven paths.
All inputs are finite; a program needn't handle non-finite values.
Results may differ from the reference program's by a relative error of at most 0.0004.
Values may be sent and summed in bfloat16 or wider, within the bound.
A program may use at most 64 MiB of HBM per device.

```python
import jax
import jax.numpy as jnp
from jax import lax

D = 4096
MODULES = 16
ROWS = 32
PATHS = 16


def draw_deltas(key, part):
    row_pos = jnp.arange(ROWS, dtype=jnp.float32) / ROWS
    col_pos = jnp.arange(D, dtype=jnp.float32) / D
    ramp = (1.0 + row_pos)[:, None] * (1.0 + col_pos)[None, :]
    log_scale = jax.random.uniform(jax.random.fold_in(key, 7), (PATHS, 1, 1), jnp.float32, -1.3862944, 1.3862944)
    path_scale = jnp.exp(log_scale)
    values = jnp.clip(jax.random.normal(key, (PATHS, ROWS, D), jnp.float32), -6.0, 6.0) * path_scale
    return (values * ramp).astype(jnp.bfloat16)


def draw_path_module(key, part):
    first = jax.random.permutation(jax.random.fold_in(key, 1), MODULES).astype(jnp.int32)
    repeated = jnp.tile(jnp.arange(MODULES, dtype=jnp.int32), 6)
    others = jax.random.permutation(jax.random.fold_in(key, 2), repeated)[:PATHS - MODULES].astype(jnp.int32)
    labels = jnp.concatenate([first, others])
    return jax.random.permutation(jax.random.fold_in(key, 3), labels).astype(jnp.int32)


def shard_levels(stream_key, dims, cuts, low, largest):
    factor_of, own = 1.0, jax.random.fold_in(stream_key, 6)
    for axis_at, shards_of in cuts:
        steps = jnp.exp(jax.random.uniform(jax.random.fold_in(own, axis_at), (shards_of,), jnp.float32, low / len(cuts), largest / len(cuts)))
        factor_of = factor_of * jnp.repeat(steps, dims[axis_at] // shards_of).reshape([-1 if axis == axis_at else 1 for axis in range(len(dims))])
    return factor_of


def normal_values(rng, extent, deviation, bound, pieces=(), kind=jnp.bfloat16):
    entries = jax.random.normal(rng, extent, jnp.float32) * deviation
    if len(pieces) > 0:
        entries = shard_levels(rng, extent, pieces, -0.22, 0.18) * entries
    return jnp.clip(entries, min=-bound, max=bound).astype(kind)


def setup_inputs(seed: int = 0) -> dict:
    keys = jax.random.split(jax.random.key(seed), 4)
    deltas = draw_deltas(jax.random.fold_in(keys[3], 71), 0)
    momentum = normal_values(keys[1], (MODULES, ROWS, D), 0.25, 4.0, ((1, 2), (2, 16)), jnp.float32)
    path_module = draw_path_module(jax.random.fold_in(keys[3], 71), 0)
    return dict(deltas=deltas, momentum=momentum, path_module=path_module)


outer_rate = 0.7
momentum_rate = 0.9
clip_ratio = 2.0

def reference(deltas, momentum, path_module):
    onehot = (path_module[:, None] == jnp.arange(MODULES, dtype=jnp.int32)[None, :]).astype(jnp.float32)
    counts = lax.optimization_barrier(jnp.sum(onehot, axis=0))
    totals = jnp.einsum('pm,prc->mrc', onehot, deltas.astype(jnp.float32), precision=lax.Precision.HIGHEST)
    outer_grad = totals / counts[:, None, None]
    norm_squares = lax.optimization_barrier(jnp.sum(outer_grad * outer_grad, axis=(1, 2)))
    limit = clip_ratio * jnp.sqrt(jnp.float32(ROWS * D))
    shrink = jnp.minimum(1.0, limit / jnp.sqrt(norm_squares + 1e-06))
    clipped = outer_grad * shrink[:, None, None]
    new_momentum = momentum_rate * momentum + clipped
    outer_step = (outer_rate * (clipped + momentum_rate * new_momentum)).astype(jnp.bfloat16)
    path_update = jnp.einsum('pm,mrc->prc', onehot, outer_step.astype(jnp.float32), precision=lax.Precision.HIGHEST).astype(jnp.bfloat16)
    return (path_update, new_momentum)
```

```python
import functools
import math

import jax
import jax.numpy as jnp
from jax import lax
from jax.experimental import pallas as pl
from jax.experimental.pallas import tpu as pltpu
from jax.sharding import PartitionSpec as P

outer_rate = 0.7
momentum_rate = 0.9
clip_ratio = 2.0
LANES = 128
MESH = pl.DeviceIdType.MESH


def kernel(
    n,
    s,
    deltas_ref,
    momentum_ref,
    path_module_ref,
    update,
    new,
    module_ref,
    own,
    momentum,
    chosen,
    pieces,
    moments,
    mine,
    pair,
    total,
    squares,
    shrink,
    load_sem,
    ready,
    pair_ready,
    piece_send,
    piece_recv,
    moment_send,
    moment_recv,
    pair_send,
    pair_recv,
    square_send,
    square_recv,
):
    me, my_shard = lax.axis_index("path"), lax.axis_index("shard")
    modules, rows, columns = momentum.shape
    width = own.shape[1]
    size = math.gcd(n, 4)
    groups = n // size
    group, place = lax.div(me, size), lax.rem(me, size)

    def device(path, shard=my_shard):
        return {"path": path, "shard": shard}

    def arrived(buffer, sem):
        pltpu.make_async_copy(buffer, buffer, sem).wait()

    def wait_for(sem, signals):
        @pl.when(signals > 0)
        def _():
            pl.semaphore_wait(sem, signals)

    def block(index):
        return pl.ds(pl.multiple_of(index * columns, columns), columns)

    def push(path):
        pltpu.make_async_remote_copy(
            src_ref=own.at[:, block(path)],
            dst_ref=pieces.at[me],
            send_sem=piece_send,
            recv_sem=piece_recv,
            device_id=device(path),
            device_id_type=MESH,
        ).start()
        pltpu.make_async_remote_copy(
            src_ref=chosen.at[path],
            dst_ref=moments.at[me],
            send_sem=moment_send,
            recv_sem=moment_recv,
            device_id=device(path),
            device_id_type=MESH,
        ).start()

    barrier = pltpu.get_barrier_semaphore()
    for path in range(1, n):
        @pl.when(path > me)
        def _():
            pl.semaphore_signal(barrier, inc=1, device_id=device(path), device_id_type=MESH)
    for shard in range(1, s):
        @pl.when(shard > my_shard)
        def _():
            pl.semaphore_signal(barrier, inc=1, device_id=device(me, shard), device_id_type=MESH)

    load_module = pltpu.make_async_copy(path_module_ref, module_ref, load_sem.at[0])
    load_own = pltpu.make_async_copy(deltas_ref.at[0], own, load_sem.at[1])
    load_momentum = pltpu.make_async_copy(momentum_ref, momentum, load_sem.at[2])
    load_module.start()
    load_own.start()
    load_momentum.start()
    load_own.wait()
    load_module.wait()
    load_momentum.wait()
    for path in range(n):
        chosen[path] = momentum[module_ref[path]]

    wait_for(barrier, me + my_shard)
    for path in range(n - 1):
        @pl.when(path < me)
        def _():
            distance = group - path // size
            pl.semaphore_signal(ready.at[distance], inc=1, device_id=device(path), device_id_type=MESH)
    for shard in range(s - 1):
        @pl.when(shard < my_shard)
        def _():
            pl.semaphore_signal(pair_ready, inc=1, device_id=device(me, shard), device_id_type=MESH)
    for path in range(n - 1):
        @pl.when(path < me)
        def _():
            push(path)

    held = own[...].astype(jnp.float32)
    by_column = jnp.sum(held * held, axis=0, keepdims=True)
    mine[...] = jnp.broadcast_to(jnp.sum(by_column, axis=1, keepdims=True), mine.shape)
    pieces[me] = own[:, block(me)]
    moments[me] = chosen[me]

    wait_for(ready.at[0], size - 1 - place)
    for at in range(1, size):
        @pl.when(at > place)
        def _():
            push(group * size + at)
    wait_for(pair_ready, s - 1 - my_shard)
    for j in range(1, s):
        shard = lax.rem(my_shard + j, s)
        pltpu.make_async_remote_copy(
            src_ref=mine,
            dst_ref=pair.at[my_shard],
            send_sem=pair_send,
            recv_sem=pair_recv,
            device_id=device(me, shard),
            device_id_type=MESH,
        ).start()
    pair[my_shard] = mine[...]
    for distance in range(1, groups):
        @pl.when(group + distance < groups)
        def _():
            pl.semaphore_wait(ready.at[distance], size)
            for at in range(size):
                push((group + distance) * size + at)

    if s > 1:
        arrived(pair.at[pl.ds(0, s - 1)], pair_recv)
    total[...] = jnp.sum(pair[...], axis=0)
    for k in range(1, n):
        path = lax.rem(me + k, n)
        pltpu.make_async_remote_copy(
            src_ref=total,
            dst_ref=squares.at[me],
            send_sem=square_send,
            recv_sem=square_recv,
            device_id=device(path),
            device_id_type=MESH,
        ).start()
    squares[me] = total[...]

    limit = clip_ratio * math.sqrt(rows * s * width)
    own_shrink = jnp.minimum(1.0, limit / jnp.sqrt(total[...] + 1e-06))
    owner = [0 for _ in range(modules)]
    for path in range(n):
        for module in range(modules):
            owner[module] = jnp.where(module_ref[path] == module, path, owner[module])

    arrived(moments.at[pl.ds(0, n - 1)], moment_recv)
    for path in range(n):
        for low in range(0, columns, LANES):
            lanes = pl.ds(low, LANES)
            at = pl.ds(path * columns + low, LANES)
            clipped = own[:, at].astype(jnp.float32) * own_shrink
            moved = momentum_rate * moments[path, :, lanes] + clipped
            update[0, :, at] = (outer_rate * (clipped + momentum_rate * moved)).astype(jnp.bfloat16)

    arrived(squares.at[pl.ds(0, n - 1)], square_recv)
    shrink[...] = jnp.minimum(1.0, limit / jnp.sqrt(squares[...] + 1e-06))
    arrived(pieces.at[pl.ds(0, n - 1)], piece_recv)
    for module in range(modules):
        factor = shrink[owner[module]]
        piece = pieces[owner[module]].astype(jnp.float32)
        for low in range(0, columns, LANES):
            lanes = pl.ds(low, LANES)
            new[module, :, lanes] = (
                momentum_rate * momentum[module, :, lanes] + piece[:, low : low + LANES] * factor
            )

    arrived(pieces.at[pl.ds(0, n - 1)], piece_send)
    arrived(moments.at[pl.ds(0, n - 1)], moment_send)
    arrived(squares.at[pl.ds(0, n - 1)], square_send)
    if s > 1:
        arrived(pair.at[pl.ds(0, s - 1)], pair_send)


def write(update, new, update_ref, new_ref, sem):
    copies = [
        pltpu.make_async_copy(update, update_ref, sem.at[0]),
        pltpu.make_async_copy(new, new_ref, sem.at[1]),
    ]
    for copy in copies:
        copy.start()
    for copy in copies:
        copy.wait()


def direct(n, s, deltas, momentum, path_module):
    modules, rows, columns = momentum.shape
    width = deltas.shape[2]
    dma = pltpu.SemaphoreType.DMA
    regular = pltpu.SemaphoreType.REGULAR
    anywhere = pl.BlockSpec(memory_space=pl.ANY)
    in_vmem = pl.BlockSpec(memory_space=pltpu.VMEM)
    held = pl.pallas_call(
        functools.partial(kernel, n, s),
        out_shape=(
            pltpu.VMEM(deltas.shape, jnp.bfloat16),
            pltpu.VMEM(momentum.shape, jnp.float32),
        ),
        in_specs=[anywhere, anywhere, anywhere],
        out_specs=(in_vmem, in_vmem),
        scratch_shapes=[
            pltpu.SMEM(path_module.shape, jnp.int32),
            pltpu.VMEM((rows, width), jnp.bfloat16),
            pltpu.VMEM((modules, rows, columns), jnp.float32),
            pltpu.VMEM((n, rows, columns), jnp.float32),
            pltpu.VMEM((n, rows, columns), jnp.bfloat16),
            pltpu.VMEM((n, rows, columns), jnp.float32),
            pltpu.VMEM((1, LANES), jnp.float32),
            pltpu.VMEM((s, 1, LANES), jnp.float32),
            pltpu.VMEM((1, LANES), jnp.float32),
            pltpu.VMEM((n, 1, LANES), jnp.float32),
            pltpu.VMEM((n, 1, LANES), jnp.float32),
            dma((3,)),
            regular((n // math.gcd(n, 4),)),
            regular,
            dma,
            dma,
            dma,
            dma,
            dma,
            dma,
            dma,
            dma,
        ],
        compiler_params=pltpu.CompilerParams(collective_id=0, has_side_effects=True),
    )(deltas, momentum, path_module)
    return pl.pallas_call(
        write,
        out_shape=(
            jax.ShapeDtypeStruct(deltas.shape, jnp.bfloat16),
            jax.ShapeDtypeStruct(momentum.shape, jnp.float32),
        ),
        in_specs=[in_vmem, in_vmem],
        out_specs=(anywhere, anywhere),
        scratch_shapes=[dma((2,))],
    )(*[pltpu.with_memory_space_constraint(x, pltpu.VMEM) for x in held])


def by_collectives(s, deltas, momentum, path_module):
    modules = momentum.shape[0]
    rows, width = deltas.shape[1:]
    onehot = path_module[:, None] == jnp.arange(modules, dtype=jnp.int32)[None, :]
    counts = jnp.sum(onehot.astype(jnp.float32), axis=0)
    pieces = lax.all_to_all(deltas, "path", split_axis=2, concat_axis=0, tiled=True)
    totals = jnp.einsum(
        "pm,prc->mrc", onehot.astype(jnp.bfloat16), pieces, preferred_element_type=jnp.float32
    )
    outer_grad = totals / counts[:, None, None]
    local_squares = jnp.sum(outer_grad * outer_grad, axis=(1, 2))
    norm_squares = lax.psum(local_squares, ("path", "shard"))
    limit = clip_ratio * math.sqrt(rows * s * width)
    shrink = jnp.minimum(1.0, limit / jnp.sqrt(norm_squares + 1e-06))
    clipped = outer_grad * shrink[:, None, None]
    new_momentum = momentum_rate * momentum + clipped
    outer_step = (outer_rate * (clipped + momentum_rate * new_momentum)).astype(jnp.bfloat16)
    chosen = jnp.take(outer_step, path_module, axis=0)
    path_update = lax.all_to_all(chosen, "path", split_axis=0, concat_axis=2, tiled=True)
    return (path_update, new_momentum)


def local(n, s, deltas, momentum, path_module):
    modules, rows, columns = momentum.shape
    aligned = columns % LANES == 0 and rows % 16 == 0
    one_path_each = path_module.shape[0] == modules == n
    if aligned and one_path_each and n > 1:
        return direct(n, s, deltas, momentum, path_module)
    return by_collectives(s, deltas, momentum, path_module)


def solution(mesh):
    return jax.shard_map(
        functools.partial(local, mesh.shape["path"], mesh.shape["shard"]),
        mesh=mesh,
        in_specs=(P("path", "shard", None), P(None, "shard", "path"), P()),
        out_specs=(P("path", "shard", None), P(None, "shard", "path")),
        check_vma=False,
    )
```

```python
import functools
import math

import jax
import jax.numpy as jnp
from jax import lax
from jax.experimental import pallas as pl
from jax.experimental.pallas import tpu as pltpu
from jax.sharding import PartitionSpec as P

outer_rate = 0.7
momentum_rate = 0.9
clip_ratio = 2.0
LANES = 128
MESH = pl.DeviceIdType.MESH


REACH = 2
REACH_FIRST = 2


def grid_of(n):
    cores = 2 if n % 2 == 0 else 1
    xs = 2 if n % 4 == 0 else 1
    return cores, xs, n // (cores * xs)


def when(condition, act):
    if condition is True:
        act()
    elif condition is not False:
        pl.when(condition)(act)


def opposite(condition):
    return not condition if isinstance(condition, bool) else jnp.logical_not(condition)


def kernel(
    n,
    s,
    deltas_ref,
    momentum_ref,
    path_module_ref,
    update,
    new,
    module_ref,
    own,
    momentum,
    chosen,
    pieces,
    moments,
    steps,
    mine,
    squares,
    shrink,
    load_sem,
    ready,
    cross,
    piece_send,
    piece_recv,
    moment_send,
    moment_recv,
    step_send,
    step_recv,
    square_send,
    square_recv,
):
    me, my_shard = lax.axis_index("path"), lax.axis_index("shard")
    modules, rows, columns = momentum.shape
    width = own.shape[1]
    cores, xs, slabs = grid_of(n)
    size = cores * xs
    core = lax.rem(me, cores)
    x = lax.rem(lax.div(me, cores), xs)
    slab = lax.div(me, size)
    limit = clip_ratio * math.sqrt(rows * s * width)
    first_shard, last_shard = my_shard == 0, my_shard == 1

    def arrived(buffer, sem):
        pltpu.make_async_copy(buffer, buffer, sem).wait()

    def signal(sem, path, shard=my_shard):
        pl.semaphore_signal(
            sem, inc=1, device_id={"path": path, "shard": shard}, device_id_type=MESH
        )

    def wait_for(sem, signals):
        when(signals > 0, lambda: pl.semaphore_wait(sem, signals))

    def block(index):
        return pl.ds(pl.multiple_of(index * columns, columns), columns)

    def send(source, target, send_sem, recv_sem, path, shard=my_shard):
        pltpu.make_async_remote_copy(
            src_ref=source,
            dst_ref=target,
            send_sem=send_sem,
            recv_sem=recv_sem,
            device_id={"path": path, "shard": shard},
            device_id_type=MESH,
        ).start()

    def push_piece(path):
        send(own.at[:, block(path)], pieces.at[me], piece_send, piece_recv.at[slab], path)

    def push_moment(path, distance):
        send(chosen.at[path], moments.at[me], moment_send.at[distance], moment_recv.at[distance], path)

    def push_square(path, shard=my_shard):
        kind = 0 if shard is my_shard else 1
        send(
            mine,
            squares.at[me, my_shard],
            square_send.at[kind],
            square_recv.at[kind * slabs + slab],
            path,
            shard,
        )

    def push_step(path, at_slab):
        send(
            steps.at[path],
            update.at[0, :, block(me)],
            step_send.at[at_slab],
            step_recv.at[slab],
            path,
        )

    def at(z, x_at, core_at):
        return z * size + x_at * cores + core_at

    def far(distance, path_slab):
        if distance >= REACH:
            return True
        if distance >= REACH_FIRST:
            return path_slab == 0
        return False

    def chip(act, z, x_at):
        for core_at in range(cores):
            act(at(z, x_at, core_at))

    def lower(condition, x_at, act):
        for distance in range(slabs - 1, 0, -1):
            def each():
                for core_at in range(cores):
                    act(at(slab - distance, x_at, core_at), distance)
            when((slab >= distance) & condition, each)

    def beside(act):
        for x_at in range(xs):
            for core_at in range(cores):
                behind = (x > x_at) | ((x == x_at) & (core > core_at))
                when(behind, lambda: act(at(slab, x_at, core_at)))

    def send_moment(path, distance):
        when(far(distance, slab - distance), lambda: push_moment(path, distance))

    barrier = pltpu.get_barrier_semaphore()
    for distance in range(slabs):
        for x_at in range(xs):
            inside = slab + distance < slabs
            if distance > 0:
                when(
                    inside & (x_at >= x),
                    lambda: chip(lambda path: signal(barrier, path), slab + distance, x_at),
                )
            else:
                for core_at in range(cores):
                    ahead = (x_at > x) | ((x_at == x) & (core_at > core))
                    when(ahead, lambda: signal(barrier, at(slab, x_at, core_at)))
            if s > 1:
                when(
                    inside & (x_at >= x) & first_shard,
                    lambda: chip(lambda path: signal(barrier, path, 1), slab + distance, x_at),
                )

    load_own = pltpu.make_async_copy(deltas_ref.at[0], own, load_sem.at[1])
    load_module = pltpu.make_async_copy(path_module_ref, module_ref, load_sem.at[0])
    load_momentum = pltpu.make_async_copy(momentum_ref, momentum, load_sem.at[2])
    load_own.start()
    load_module.start()
    load_momentum.start()

    before = (slab * (x + 1) + x) * cores + core
    wait_for(barrier, before + my_shard * (slab + 1) * (x + 1) * cores)
    for x_at in range(xs):
        lower(
            x >= x_at, x_at, lambda path, distance: signal(ready.at[distance * xs + x], path)
        )
    beside(lambda path: signal(ready.at[x], path))
    if s > 1:
        for x_at in range(xs):
            lower(
                last_shard & (x >= x_at),
                x_at,
                lambda path, distance: signal(cross.at[distance * xs + x], path, 0),
            )
            when(
                last_shard & (x >= x_at),
                lambda: chip(lambda path: signal(cross.at[x], path, 0), slab, x_at),
            )

    load_own.wait()
    held = own[...].astype(jnp.float32)
    by_column = jnp.sum(held * held, axis=0, keepdims=True)
    mine[...] = jnp.broadcast_to(jnp.sum(by_column, axis=1, keepdims=True), mine.shape)
    for x_at in range(xs):
        lower(x >= x_at, x_at, lambda path, distance: push_square(path))
        if s > 1:
            lower(
                last_shard & (x >= x_at), x_at, lambda path, distance: push_square(path, 0)
            )
            when(
                last_shard & (x >= x_at),
                lambda: chip(lambda path: push_square(path, 0), slab, x_at),
            )
    beside(push_square)
    for x_at in range(xs):
        lower(x >= x_at, x_at, lambda path, distance: push_piece(path))
    beside(push_piece)
    squares[me, my_shard] = mine[...]

    load_module.wait()
    load_momentum.wait()
    for distance in range(1, slabs):
        def choose():
            for b in range(size):
                path = (slab - distance) * size + b
                chosen[path] = momentum[module_ref[path]]
        if far(distance, slab - distance) is not False:
            when((slab >= distance) & far(distance, slab - distance), choose)
    pieces[me] = own[:, block(me)]

    if s > 1:
        def across():
            pl.semaphore_wait(cross.at[x], cores)
            for x_at in range(xs):
                lower(x >= x_at, x_at, lambda path, distance: push_square(path, 1))
                when(
                    x >= x_at,
                    lambda: chip(lambda path: push_square(path, 1), slab, x_at),
                )
        when(first_shard, across)

    for x_at in range(xs):
        def same_chip():
            wait_for(ready.at[x_at], cores - 1 - core)
            for core_at in range(1, cores):
                def give():
                    push_square(at(slab, x_at, core_at))
                    push_piece(at(slab, x_at, core_at))
                when(core_at > core, give)

        def next_chip():
            pl.semaphore_wait(ready.at[x_at], cores)
            lower(True, x_at, lambda path, distance: push_square(path))
            chip(push_square, slab, x_at)
            if s > 1:
                def over():
                    lower(True, x_at, lambda path, distance: push_square(path, 0))
                    chip(lambda path: push_square(path, 0), slab, x_at)
                when(last_shard, over)

            lower(True, x_at, lambda path, distance: push_piece(path))
            chip(push_piece, slab, x_at)

        when(x_at == x, same_chip)
        when(x_at > x, next_chip)

    if s > 1:
        for x_at in range(1, xs):
            def rest():
                pl.semaphore_wait(cross.at[x_at], cores)
                lower(True, x_at, lambda path, distance: push_square(path, 1))
                chip(lambda path: push_square(path, 1), slab, x_at)
            when((x_at > x) & first_shard, rest)

    def push_above(distance):
        def go():
            def give(x_at):
                chip(push_square, slab + distance, x_at)
                if s > 1:
                    when(
                        last_shard,
                        lambda: chip(lambda path: push_square(path, 0), slab + distance, x_at),
                    )
                chip(push_piece, slab + distance, x_at)

            for x_at in range(xs):
                def known():
                    pl.semaphore_wait(ready.at[distance * xs + x_at], cores)
                    give(x_at)
                when(x_at >= x, known)
                for low in range(x_at):
                    when(x_at == x, lambda: give(low))
        when(slab + distance < slabs, go)

    def cross_above(distance):
        def go():
            def give(x_at):
                chip(lambda path: push_square(path, 1), slab + distance, x_at)

            for x_at in range(xs):
                def known():
                    pl.semaphore_wait(cross.at[distance * xs + x_at], cores)
                    give(x_at)
                when(x_at >= x, known)
                for low in range(x_at):
                    when(x_at == x, lambda: give(low))
        when((slab + distance < slabs) & first_shard, go)

    for distance in range(1, slabs):
        push_above(distance)
        if s > 1:
            cross_above(distance)

    def step_of(clipped, previous):
        moved = momentum_rate * previous + clipped
        return (outer_rate * (clipped + momentum_rate * moved)).astype(jnp.bfloat16)

    def collect(source, count, answer):
        base = source * size
        arrived(pieces.at[pl.ds(0, count)], piece_recv.at[source])
        arrived(squares.at[pl.ds(0, count), 0], square_recv.at[source])
        if s > 1:
            arrived(squares.at[pl.ds(0, size), 0], square_recv.at[slabs + source])
        norm_squares = jnp.sum(squares[pl.ds(base, size)], axis=1)
        shrink[pl.ds(base, size)] = jnp.minimum(1.0, limit / jnp.sqrt(norm_squares + 1e-06))

        def reply():
            for b in range(size):
                module = module_ref[base + b]
                factor = shrink[base + b]
                for low in range(0, columns, LANES):
                    lanes = pl.ds(low, LANES)
                    clipped = pieces[base + b, :, lanes].astype(jnp.float32) * factor
                    steps[base + b, :, lanes] = step_of(clipped, momentum[module, :, lanes])
            for b in range(size):
                when(base + b != me, lambda: push_step(base + b, source))
        when(answer, reply)

    collect(slab, size - 1, True)
    for x_at in range(xs):
        lower(True, x_at, send_moment)

    update[0, :, block(me)] = steps[me]
    for distance in range(1, slabs):
        when(
            slab + distance < slabs,
            lambda: collect(slab + distance, size, True),
        )
        answer = opposite(far(distance, slab - distance))
        when(
            slab >= distance,
            lambda: collect(slab - distance, size, answer),
        )

    for distance in range(1, slabs):
        def receive():
            arrived(moments.at[pl.ds(0, size)], moment_recv.at[distance])
            factor = shrink[me]
            for b in range(size):
                owner = (slab + distance) * size + b
                for low in range(0, columns, LANES):
                    lanes = pl.ds(pl.multiple_of(owner * columns + low, LANES), LANES)
                    clipped = own[:, lanes].astype(jnp.float32) * factor
                    update[0, :, lanes] = step_of(clipped, moments[owner, :, pl.ds(low, LANES)])
        if far(distance, slab) is not False:
            when((slab + distance < slabs) & far(distance, slab), receive)

    source = [0 for _ in range(modules)]
    for path in range(n):
        for module in range(modules):
            source[module] = jnp.where(module_ref[path] == module, path, source[module])
    for module in range(modules):
        factor = shrink[source[module]]
        for low in range(0, columns, LANES):
            lanes = pl.ds(low, LANES)
            clipped = pieces[source[module], :, lanes].astype(jnp.float32) * factor
            new[module, :, lanes] = momentum_rate * momentum[module, :, lanes] + clipped

    arrived(pieces.at[pl.ds(0, n - 1)], piece_send)
    arrived(squares.at[pl.ds(0, n - 1), 0], square_send.at[0])
    if s > 1:
        arrived(squares.at[:, 0], square_send.at[1])
    arrived(steps.at[pl.ds(0, size - 1)], step_send.at[slab])
    for distance in range(1, slabs):
        above, below = slab + distance, slab - distance
        sent = far(distance, below)
        when(above < slabs, lambda: arrived(steps.at[pl.ds(0, size)], step_send.at[above]))
        if sent is not False:
            when(
                (below >= 0) & sent,
                lambda: arrived(moments.at[pl.ds(0, size)], moment_send.at[distance]),
            )
        if sent is not True:
            when(
                (below >= 0) & opposite(sent),
                lambda: arrived(steps.at[pl.ds(0, size)], step_send.at[below]),
            )
    arrived(steps.at[pl.ds(0, size - 1)], step_recv.at[slab])
    for distance in range(1, slabs):
        above, below = slab + distance, slab - distance
        got = far(distance, slab)
        when(below >= 0, lambda: arrived(steps.at[pl.ds(0, size)], step_recv.at[below]))
        if got is not True:
            when(
                (above < slabs) & opposite(got),
                lambda: arrived(steps.at[pl.ds(0, size)], step_recv.at[above]),
            )


def write(update, new, update_ref, new_ref, sem):
    copies = [
        pltpu.make_async_copy(update, update_ref, sem.at[0]),
        pltpu.make_async_copy(new, new_ref, sem.at[1]),
    ]
    for copy in copies:
        copy.start()
    for copy in copies:
        copy.wait()


def direct(n, s, deltas, momentum, path_module):
    modules, rows, columns = momentum.shape
    width = deltas.shape[2]
    _, xs, slabs = grid_of(n)
    dma = pltpu.SemaphoreType.DMA
    regular = pltpu.SemaphoreType.REGULAR
    anywhere = pl.BlockSpec(memory_space=pl.ANY)
    in_vmem = pl.BlockSpec(memory_space=pltpu.VMEM)
    held = pl.pallas_call(
        functools.partial(kernel, n, s),
        out_shape=(
            pltpu.VMEM(deltas.shape, jnp.bfloat16),
            pltpu.VMEM(momentum.shape, jnp.float32),
        ),
        in_specs=[anywhere, anywhere, anywhere],
        out_specs=(in_vmem, in_vmem),
        scratch_shapes=[
            pltpu.SMEM(path_module.shape, jnp.int32),
            pltpu.VMEM((rows, width), jnp.bfloat16),
            pltpu.VMEM((modules, rows, columns), jnp.float32),
            pltpu.VMEM((n, rows, columns), jnp.float32),
            pltpu.VMEM((n, rows, columns), jnp.bfloat16),
            pltpu.VMEM((n, rows, columns), jnp.float32),
            pltpu.VMEM((n, rows, columns), jnp.bfloat16),
            pltpu.VMEM((1, LANES), jnp.float32),
            pltpu.VMEM((n, s, 1, LANES), jnp.float32),
            pltpu.VMEM((n, 1, LANES), jnp.float32),
            dma((3,)),
            regular((slabs * xs,)),
            regular((slabs * xs,)),
            dma,
            dma((slabs,)),
            dma((slabs,)),
            dma((slabs,)),
            dma((slabs,)),
            dma((slabs,)),
            dma((2,)),
            dma((2 * slabs,)),
        ],
        compiler_params=pltpu.CompilerParams(collective_id=0, has_side_effects=True),
    )(deltas, momentum, path_module)
    return pl.pallas_call(
        write,
        out_shape=(
            jax.ShapeDtypeStruct(deltas.shape, jnp.bfloat16),
            jax.ShapeDtypeStruct(momentum.shape, jnp.float32),
        ),
        in_specs=[in_vmem, in_vmem],
        out_specs=(anywhere, anywhere),
        scratch_shapes=[dma((2,))],
    )(*[pltpu.with_memory_space_constraint(x, pltpu.VMEM) for x in held])


def by_collectives(s, deltas, momentum, path_module):
    modules = momentum.shape[0]
    rows, width = deltas.shape[1:]
    onehot = path_module[:, None] == jnp.arange(modules, dtype=jnp.int32)[None, :]
    counts = jnp.sum(onehot.astype(jnp.float32), axis=0)
    pieces = lax.all_to_all(deltas, "path", split_axis=2, concat_axis=0, tiled=True)
    totals = jnp.einsum(
        "pm,prc->mrc", onehot.astype(jnp.bfloat16), pieces, preferred_element_type=jnp.float32
    )
    outer_grad = totals / counts[:, None, None]
    local_squares = jnp.sum(outer_grad * outer_grad, axis=(1, 2))
    norm_squares = lax.psum(local_squares, ("path", "shard"))
    limit = clip_ratio * math.sqrt(rows * s * width)
    shrink = jnp.minimum(1.0, limit / jnp.sqrt(norm_squares + 1e-06))
    clipped = outer_grad * shrink[:, None, None]
    new_momentum = momentum_rate * momentum + clipped
    outer_step = (outer_rate * (clipped + momentum_rate * new_momentum)).astype(jnp.bfloat16)
    chosen = jnp.take(outer_step, path_module, axis=0)
    path_update = lax.all_to_all(chosen, "path", split_axis=0, concat_axis=2, tiled=True)
    return (path_update, new_momentum)


def local(n, s, deltas, momentum, path_module):
    modules, rows, columns = momentum.shape
    aligned = columns % LANES == 0 and rows % 16 == 0
    one_path_each = path_module.shape[0] == modules == n
    if aligned and one_path_each and n > 1 and s <= 2:
        return direct(n, s, deltas, momentum, path_module)
    return by_collectives(s, deltas, momentum, path_module)


def solution(mesh):
    return jax.shard_map(
        functools.partial(local, mesh.shape["path"], mesh.shape["shard"]),
        mesh=mesh,
        in_specs=(P("path", "shard", None), P(None, "shard", "path"), P()),
        out_specs=(P("path", "shard", None), P(None, "shard", "path")),
        check_vma=False,
    )
```

```python
import functools
import math

import jax
import jax.numpy as jnp
from jax import lax
from jax.experimental import pallas as pl
from jax.experimental.pallas import tpu as pltpu
from jax.sharding import PartitionSpec as P

outer_rate = 0.7
momentum_rate = 0.9
clip_ratio = 2.0
LANES = 128
MESH = pl.DeviceIdType.MESH


REACH = 3
REACH_FIRST = 2


def grid_of(n):
    cores = 2 if n % 2 == 0 else 1
    xs = 2 if n % 4 == 0 else 1
    return cores, xs, n // (cores * xs)


def when(condition, act):
    if condition is True:
        act()
    elif condition is not False:
        pl.when(condition)(act)


def tally_rows(rows, columns):
    return rows * columns * 2 // (LANES * 4), rows * columns * 4 // (LANES * 4)


def opposite(condition):
    return not condition if isinstance(condition, bool) else jnp.logical_not(condition)


def kernel(
    n,
    s,
    deltas_ref,
    momentum_ref,
    path_module_ref,
    update,
    new,
    module_ref,
    own,
    momentum,
    chosen,
    pieces,
    moments,
    steps,
    mine,
    squares,
    shrink,
    tally,
    load_sem,
    ready,
    cross,
    left,
    came,
    moment_came,
    step_came,
):
    me, my_shard = lax.axis_index("path"), lax.axis_index("shard")
    modules, rows, columns = momentum.shape
    width = own.shape[1]
    cores, xs, slabs = grid_of(n)
    size = cores * xs
    core = lax.rem(me, cores)
    x = lax.rem(lax.div(me, cores), xs)
    slab = lax.div(me, size)
    limit = clip_ratio * math.sqrt(rows * s * width)
    piece_rows, moment_rows = tally_rows(rows, columns)
    first_shard, last_shard = my_shard == 0, my_shard == 1

    def arrived(count, sem):
        if count > 0:
            part = tally.at[pl.ds(0, count)]
            pltpu.make_async_copy(part, part, sem).wait()

    def signal(sem, path, shard=my_shard):
        pl.semaphore_signal(
            sem, inc=1, device_id={"path": path, "shard": shard}, device_id_type=MESH
        )

    def wait_for(sem, signals):
        when(signals > 0, lambda: pl.semaphore_wait(sem, signals))

    def block(index):
        return pl.ds(pl.multiple_of(index * columns, columns), columns)

    def send(source, target, recv_sem, path, shard=my_shard):
        pltpu.make_async_remote_copy(
            src_ref=source,
            dst_ref=target,
            send_sem=left,
            recv_sem=recv_sem,
            device_id={"path": path, "shard": shard},
            device_id_type=MESH,
        ).start()

    def push_piece(path):
        send(own.at[:, block(path)], pieces.at[me], came.at[slab], path)

    def push_moment(path, distance):
        send(chosen.at[path], moments.at[me], moment_came, path)

    def push_square(path, shard=my_shard):
        send(mine, squares.at[me * s + my_shard], came.at[slab], path, shard)

    def push_step(path):
        send(steps.at[path], update.at[0, :, block(me)], step_came, path)

    def at(z, x_at, core_at):
        return z * size + x_at * cores + core_at

    def far(distance, path_slab):
        if distance >= REACH:
            return True
        if distance >= REACH_FIRST:
            return path_slab == 0
        return False

    def chip(act, z, x_at):
        for core_at in range(cores):
            act(at(z, x_at, core_at))

    def lower(condition, x_at, act):
        for distance in range(slabs - 1, 0, -1):
            def each():
                for core_at in range(cores):
                    act(at(slab - distance, x_at, core_at), distance)
            when((slab >= distance) & condition, each)

    def beside(act):
        for x_at in range(xs):
            for core_at in range(cores):
                behind = (x > x_at) | ((x == x_at) & (core > core_at))
                when(behind, lambda: act(at(slab, x_at, core_at)))

    def send_moment(path, distance):
        when(far(distance, slab - distance), lambda: push_moment(path, distance))

    load_own = pltpu.make_async_copy(deltas_ref.at[0], own, load_sem.at[1])
    load_module = pltpu.make_async_copy(path_module_ref, module_ref, load_sem.at[0])
    load_momentum = pltpu.make_async_copy(momentum_ref, momentum, load_sem.at[2])
    load_own.start()
    load_module.start()
    load_momentum.start()

    barrier = pltpu.get_barrier_semaphore()
    for distance in range(slabs):
        for x_at in range(xs):
            inside = slab + distance < slabs
            if distance > 0:
                when(
                    inside & (x_at >= x),
                    lambda: chip(lambda path: signal(barrier, path), slab + distance, x_at),
                )
            else:
                for core_at in range(cores):
                    ahead = (x_at > x) | ((x_at == x) & (core_at > core))
                    when(ahead, lambda: signal(barrier, at(slab, x_at, core_at)))
            if s > 1:
                when(
                    inside & (x_at >= x) & first_shard,
                    lambda: chip(lambda path: signal(barrier, path, 1), slab + distance, x_at),
                )

    before = (slab * (x + 1) + x) * cores + core
    wait_for(barrier, before + my_shard * (slab + 1) * (x + 1) * cores)
    for x_at in range(xs):
        lower(
            x >= x_at, x_at, lambda path, distance: signal(ready.at[distance * xs + x], path)
        )
    beside(lambda path: signal(ready.at[x], path))
    if s > 1:
        for x_at in range(xs):
            lower(
                last_shard & (x >= x_at),
                x_at,
                lambda path, distance: signal(cross.at[distance * xs + x], path, 0),
            )
            when(
                last_shard & (x >= x_at),
                lambda: chip(lambda path: signal(cross.at[x], path, 0), slab, x_at),
            )

    load_own.wait()
    held = own[...].astype(jnp.float32)
    by_column = jnp.sum(held * held, axis=0, keepdims=True)
    mine[...] = jnp.broadcast_to(jnp.sum(by_column, axis=1, keepdims=True), mine.shape)
    for x_at in range(xs):
        lower(x >= x_at, x_at, lambda path, distance: push_square(path))
        if s > 1:
            lower(
                last_shard & (x >= x_at), x_at, lambda path, distance: push_square(path, 0)
            )
            when(
                last_shard & (x >= x_at),
                lambda: chip(lambda path: push_square(path, 0), slab, x_at),
            )
    beside(push_square)
    for x_at in range(xs):
        lower(x >= x_at, x_at, lambda path, distance: push_piece(path))
    beside(push_piece)
    squares[me * s + my_shard] = mine[...]

    load_module.wait()
    load_momentum.wait()
    for distance in range(1, slabs):
        def choose():
            for b in range(size):
                path = (slab - distance) * size + b
                chosen[path] = momentum[module_ref[path]]
        if far(distance, slab - distance) is not False:
            when((slab >= distance) & far(distance, slab - distance), choose)
    pieces[me] = own[:, block(me)]

    if s > 1:
        def across():
            pl.semaphore_wait(cross.at[x], cores)
            for x_at in range(xs):
                lower(x >= x_at, x_at, lambda path, distance: push_square(path, 1))
                when(
                    x >= x_at,
                    lambda: chip(lambda path: push_square(path, 1), slab, x_at),
                )
        when(first_shard, across)

    for x_at in range(xs):
        def same_chip():
            wait_for(ready.at[x_at], cores - 1 - core)
            for core_at in range(1, cores):
                def give():
                    push_square(at(slab, x_at, core_at))
                    push_piece(at(slab, x_at, core_at))
                when(core_at > core, give)

        def next_chip():
            pl.semaphore_wait(ready.at[x_at], cores)
            lower(True, x_at, lambda path, distance: push_square(path))
            chip(push_square, slab, x_at)
            if s > 1:
                def over():
                    lower(True, x_at, lambda path, distance: push_square(path, 0))
                    chip(lambda path: push_square(path, 0), slab, x_at)
                when(last_shard, over)

            lower(True, x_at, lambda path, distance: push_piece(path))
            chip(push_piece, slab, x_at)

        when(x_at == x, same_chip)
        when(x_at > x, next_chip)

    if s > 1:
        for x_at in range(1, xs):
            def rest():
                pl.semaphore_wait(cross.at[x_at], cores)
                lower(True, x_at, lambda path, distance: push_square(path, 1))
                chip(lambda path: push_square(path, 1), slab, x_at)
            when((x_at > x) & first_shard, rest)

    def push_above(distance):
        def go():
            def give(x_at):
                chip(push_square, slab + distance, x_at)
                if s > 1:
                    when(
                        last_shard,
                        lambda: chip(lambda path: push_square(path, 0), slab + distance, x_at),
                    )
                chip(push_piece, slab + distance, x_at)

            for x_at in range(xs):
                def known():
                    pl.semaphore_wait(ready.at[distance * xs + x_at], cores)
                    give(x_at)
                when(x_at >= x, known)
                for low in range(x_at):
                    when(x_at == x, lambda: give(low))
        when(slab + distance < slabs, go)

    def cross_above(distance):
        def go():
            def give(x_at):
                chip(lambda path: push_square(path, 1), slab + distance, x_at)

            for x_at in range(xs):
                def known():
                    pl.semaphore_wait(cross.at[distance * xs + x_at], cores)
                    give(x_at)
                when(x_at >= x, known)
                for low in range(x_at):
                    when(x_at == x, lambda: give(low))
        when((slab + distance < slabs) & first_shard, go)

    for distance in range(1, slabs):
        push_above(distance)
        if s > 1:
            cross_above(distance)

    for x_at in range(xs):
        lower(True, x_at, lambda path, distance: send_moment(path, distance) if distance in (3,) else None)

    def step_of(clipped, previous):
        moved = momentum_rate * previous + clipped
        return (outer_rate * (clipped + momentum_rate * moved)).astype(jnp.bfloat16)

    def collect(source, count, answer):
        base = source * size
        arrived(count * piece_rows + count * s + (size - count) * (s - 1), came.at[source])
        both = squares[pl.ds(base * s, size * s)].reshape(size, s, 1, LANES)
        norm_squares = jnp.sum(both, axis=1)
        shrink[pl.ds(base, size)] = jnp.minimum(1.0, limit / jnp.sqrt(norm_squares + 1e-06))

        def reply():
            for b in range(size):
                module = module_ref[base + b]
                factor = shrink[base + b]
                for low in range(0, columns, LANES):
                    lanes = pl.ds(low, LANES)
                    clipped = pieces[base + b, :, lanes].astype(jnp.float32) * factor
                    steps[base + b, :, lanes] = step_of(clipped, momentum[module, :, lanes])
            for b in range(size):
                when(base + b != me, lambda: push_step(base + b))
        when(answer, reply)

    collect(slab, size - 1, True)
    for x_at in range(xs):
        lower(True, x_at, lambda path, distance: send_moment(path, distance) if distance in (1, 2) else None)

    update[0, :, block(me)] = steps[me]
    for distance in range(1, slabs):
        answer = opposite(far(distance, slab - distance))
        when(
            slab >= distance,
            lambda: collect(slab - distance, size, answer),
        )
    for distance in range(1, slabs):
        when(
            slab + distance < slabs,
            lambda: collect(slab + distance, size, True),
        )

    source = [0 for _ in range(modules)]
    for path in range(n):
        for module in range(modules):
            source[module] = jnp.where(module_ref[path] == module, path, source[module])
    for module in range(modules):
        factor = shrink[source[module]]
        for low in range(0, columns, LANES):
            lanes = pl.ds(low, LANES)
            clipped = pieces[source[module], :, lanes].astype(jnp.float32) * factor
            new[module, :, lanes] = momentum_rate * momentum[module, :, lanes] + clipped

    def finish(at_slab):
        owners = [z for z in range(at_slab + 1, slabs) if far(z - at_slab, at_slab)]
        arrived(len(owners) * size * moment_rows, moment_came)
        factor = shrink[me]
        for owner in [z * size + b for z in owners for b in range(size)]:
            for low in range(0, columns, LANES):
                lanes = pl.ds(owner * columns + low, LANES)
                clipped = own[:, lanes].astype(jnp.float32) * factor
                update[0, :, lanes] = step_of(clipped, moments[owner, :, pl.ds(low, LANES)])
        told = [z for z in range(at_slab) if far(at_slab - z, z)]
        sent = (n - 1) * piece_rows + n * s - 1 + len(told) * size * moment_rows
        sent += ((slabs - len(told)) * size - 1) * piece_rows
        arrived(sent, left)
        arrived(((slabs - len(owners)) * size - 1) * piece_rows, step_came)

    for at_slab in range(slabs):
        when(slab == at_slab, lambda: finish(at_slab))


def write(update, new, update_ref, new_ref, sem):
    copies = [
        pltpu.make_async_copy(update, update_ref, sem.at[0]),
        pltpu.make_async_copy(new, new_ref, sem.at[1]),
    ]
    for copy in copies:
        copy.start()
    for copy in copies:
        copy.wait()


def direct(n, s, deltas, momentum, path_module):
    modules, rows, columns = momentum.shape
    width = deltas.shape[2]
    _, xs, slabs = grid_of(n)
    piece_rows, moment_rows = tally_rows(rows, columns)
    dma = pltpu.SemaphoreType.DMA
    regular = pltpu.SemaphoreType.REGULAR
    anywhere = pl.BlockSpec(memory_space=pl.ANY)
    in_vmem = pl.BlockSpec(memory_space=pltpu.VMEM)
    held = pl.pallas_call(
        functools.partial(kernel, n, s),
        out_shape=(
            pltpu.VMEM(deltas.shape, jnp.bfloat16),
            pltpu.VMEM(momentum.shape, jnp.float32),
        ),
        in_specs=[anywhere, anywhere, anywhere],
        out_specs=(in_vmem, in_vmem),
        scratch_shapes=[
            pltpu.SMEM(path_module.shape, jnp.int32),
            pltpu.VMEM((rows, width), jnp.bfloat16),
            pltpu.VMEM((modules, rows, columns), jnp.float32),
            pltpu.VMEM((n, rows, columns), jnp.float32),
            pltpu.VMEM((n, rows, columns), jnp.bfloat16),
            pltpu.VMEM((n, rows, columns), jnp.float32),
            pltpu.VMEM((n, rows, columns), jnp.bfloat16),
            pltpu.VMEM((1, LANES), jnp.float32),
            pltpu.VMEM((n * s, 1, LANES), jnp.float32),
            pltpu.VMEM((n, 1, LANES), jnp.float32),
            pltpu.VMEM((n * (2 * piece_rows + moment_rows + s), 1, LANES), jnp.float32),
            dma((3,)),
            regular((slabs * xs,)),
            regular((slabs * xs,)),
            dma,
            dma((slabs,)),
            dma,
            dma,
        ],
        compiler_params=pltpu.CompilerParams(collective_id=0, has_side_effects=True),
    )(deltas, momentum, path_module)
    return pl.pallas_call(
        write,
        out_shape=(
            jax.ShapeDtypeStruct(deltas.shape, jnp.bfloat16),
            jax.ShapeDtypeStruct(momentum.shape, jnp.float32),
        ),
        in_specs=[in_vmem, in_vmem],
        out_specs=(anywhere, anywhere),
        scratch_shapes=[dma((2,))],
    )(*[pltpu.with_memory_space_constraint(x, pltpu.VMEM) for x in held])


def by_collectives(s, deltas, momentum, path_module):
    modules = momentum.shape[0]
    rows, width = deltas.shape[1:]
    onehot = path_module[:, None] == jnp.arange(modules, dtype=jnp.int32)[None, :]
    counts = jnp.sum(onehot.astype(jnp.float32), axis=0)
    pieces = lax.all_to_all(deltas, "path", split_axis=2, concat_axis=0, tiled=True)
    totals = jnp.einsum(
        "pm,prc->mrc", onehot.astype(jnp.bfloat16), pieces, preferred_element_type=jnp.float32
    )
    outer_grad = totals / counts[:, None, None]
    local_squares = jnp.sum(outer_grad * outer_grad, axis=(1, 2))
    norm_squares = lax.psum(local_squares, ("path", "shard"))
    limit = clip_ratio * math.sqrt(rows * s * width)
    shrink = jnp.minimum(1.0, limit / jnp.sqrt(norm_squares + 1e-06))
    clipped = outer_grad * shrink[:, None, None]
    new_momentum = momentum_rate * momentum + clipped
    outer_step = (outer_rate * (clipped + momentum_rate * new_momentum)).astype(jnp.bfloat16)
    chosen = jnp.take(outer_step, path_module, axis=0)
    path_update = lax.all_to_all(chosen, "path", split_axis=0, concat_axis=2, tiled=True)
    return (path_update, new_momentum)


def local(n, s, deltas, momentum, path_module):
    modules, rows, columns = momentum.shape
    aligned = columns % LANES == 0 and rows % 16 == 0
    one_path_each = path_module.shape[0] == modules == n
    if aligned and one_path_each and n > 1 and s <= 2:
        return direct(n, s, deltas, momentum, path_module)
    return by_collectives(s, deltas, momentum, path_module)


def solution(mesh):
    return jax.shard_map(
        functools.partial(local, mesh.shape["path"], mesh.shape["shard"]),
        mesh=mesh,
        in_specs=(P("path", "shard", None), P(None, "shard", "path"), P()),
        out_specs=(P("path", "shard", None), P(None, "shard", "path")),
        check_vma=False,
    )
```

```python
import functools
import math

import jax
import jax.numpy as jnp
from jax import lax
from jax.experimental import pallas as pl
from jax.experimental.pallas import tpu as pltpu
from jax.sharding import PartitionSpec as P

outer_rate = 0.7
momentum_rate = 0.9
clip_ratio = 2.0
LANES = 128
MESH = pl.DeviceIdType.MESH


REACH = 2
REACH_FIRST = 1


def grid_of(n):
    cores = 2 if n % 2 == 0 else 1
    xs = 2 if n % 4 == 0 else 1
    return cores, xs, n // (cores * xs)


def when(condition, act):
    if condition is True:
        act()
    elif condition is not False:
        pl.when(condition)(act)


def tally_rows(rows, columns):
    return rows * columns * 2 // (LANES * 4), rows * columns * 4 // (LANES * 4)


def opposite(condition):
    return not condition if isinstance(condition, bool) else jnp.logical_not(condition)


def kernel(
    n,
    s,
    deltas_ref,
    momentum_ref,
    path_module_ref,
    update,
    new,
    module_ref,
    own,
    momentum,
    chosen,
    pieces,
    moments,
    steps,
    mine,
    squares,
    shrink,
    tally,
    load_sem,
    ready,
    cross,
    left,
    came,
    moment_came,
    step_came,
):
    me, my_shard = lax.axis_index("path"), lax.axis_index("shard")
    modules, rows, columns = momentum.shape
    width = own.shape[1]
    cores, xs, slabs = grid_of(n)
    size = cores * xs
    core = lax.rem(me, cores)
    x = lax.rem(lax.div(me, cores), xs)
    slab = lax.div(me, size)
    limit = clip_ratio * math.sqrt(rows * s * width)
    piece_rows, moment_rows = tally_rows(rows, columns)
    first_shard, last_shard = my_shard == 0, my_shard == 1

    def arrived(count, sem):
        if count > 0:
            part = tally.at[pl.ds(0, count)]
            pltpu.make_async_copy(part, part, sem).wait()

    def signal(sem, path, shard=my_shard):
        pl.semaphore_signal(
            sem, inc=1, device_id={"path": path, "shard": shard}, device_id_type=MESH
        )

    def wait_for(sem, signals):
        when(signals > 0, lambda: pl.semaphore_wait(sem, signals))

    def block(index):
        return pl.ds(pl.multiple_of(index * columns, columns), columns)

    def send(source, target, recv_sem, path, shard=my_shard):
        pltpu.make_async_remote_copy(
            src_ref=source,
            dst_ref=target,
            send_sem=left,
            recv_sem=recv_sem,
            device_id={"path": path, "shard": shard},
            device_id_type=MESH,
        ).start()

    def push_piece(path):
        send(own.at[:, block(path)], pieces.at[me], came.at[slab], path)

    def push_moment(path, distance):
        send(chosen.at[path], moments.at[me], moment_came, path)

    def push_square(path, shard=my_shard):
        send(mine, squares.at[me * s + my_shard], came.at[slab], path, shard)

    def push_step(path):
        send(steps.at[path], update.at[0, :, block(me)], step_came, path)

    def at(z, x_at, core_at):
        return z * size + x_at * cores + core_at

    def far(distance, path_slab):
        if distance >= REACH:
            return True
        if distance >= REACH_FIRST:
            return path_slab == 0
        return False

    def chip(act, z, x_at):
        for core_at in range(cores):
            act(at(z, x_at, core_at))

    def lower(condition, x_at, act):
        for distance in range(slabs - 1, 0, -1):
            def each():
                for core_at in range(cores):
                    act(at(slab - distance, x_at, core_at), distance)
            when((slab >= distance) & condition, each)

    def beside(act):
        for x_at in range(xs):
            for core_at in range(cores):
                behind = (x > x_at) | ((x == x_at) & (core > core_at))
                when(behind, lambda: act(at(slab, x_at, core_at)))

    def send_moment(path, distance):
        when(far(distance, slab - distance), lambda: push_moment(path, distance))

    load_own = pltpu.make_async_copy(deltas_ref.at[0], own, load_sem.at[1])
    load_module = pltpu.make_async_copy(path_module_ref, module_ref, load_sem.at[0])
    load_momentum = pltpu.make_async_copy(momentum_ref, momentum, load_sem.at[2])
    load_own.start()
    load_module.start()
    load_momentum.start()

    barrier = pltpu.get_barrier_semaphore()
    for distance in range(slabs):
        for x_at in range(xs):
            inside = slab + distance < slabs
            if distance > 0:
                when(
                    inside & (x_at >= x),
                    lambda: chip(lambda path: signal(barrier, path), slab + distance, x_at),
                )
            else:
                for core_at in range(cores):
                    ahead = (x_at > x) | ((x_at == x) & (core_at > core))
                    when(ahead, lambda: signal(barrier, at(slab, x_at, core_at)))
            if s > 1:
                when(
                    inside & (x_at >= x) & first_shard,
                    lambda: chip(lambda path: signal(barrier, path, 1), slab + distance, x_at),
                )

    before = (slab * (x + 1) + x) * cores + core
    wait_for(barrier, before + my_shard * (slab + 1) * (x + 1) * cores)
    for x_at in range(xs):
        lower(
            x >= x_at, x_at, lambda path, distance: signal(ready.at[distance * xs + x], path)
        )
    beside(lambda path: signal(ready.at[x], path))
    if s > 1:
        for x_at in range(xs):
            lower(
                last_shard & (x >= x_at),
                x_at,
                lambda path, distance: signal(cross.at[xs - 1 + distance], path, 0),
            )
            when(
                last_shard & (x >= x_at),
                lambda: chip(lambda path: signal(cross.at[x], path, 0), slab, x_at),
            )

    load_own.wait()
    held = own[...].astype(jnp.float32)
    by_column = jnp.sum(held * held, axis=0, keepdims=True)
    mine[...] = jnp.broadcast_to(jnp.sum(by_column, axis=1, keepdims=True), mine.shape)
    for x_at in range(xs):
        lower(x >= x_at, x_at, lambda path, distance: push_square(path))
        if s > 1:
            lower(
                last_shard & (x >= x_at), x_at, lambda path, distance: push_square(path, 0)
            )
            when(
                last_shard & (x >= x_at),
                lambda: chip(lambda path: push_square(path, 0), slab, x_at),
            )
    beside(push_square)
    for x_at in range(xs):
        lower(x >= x_at, x_at, lambda path, distance: push_piece(path))
    beside(push_piece)
    squares[me * s + my_shard] = mine[...]

    load_module.wait()
    load_momentum.wait()
    for distance in range(1, slabs):
        def choose():
            for b in range(size):
                path = (slab - distance) * size + b
                chosen[path] = momentum[module_ref[path]]
        if far(distance, slab - distance) is not False:
            when((slab >= distance) & far(distance, slab - distance), choose)
    for x_at in range(xs):
        lower(
            x >= x_at,
            x_at,
            lambda path, distance: send_moment(path, distance) if distance in (1,) else None,
        )
    pieces[me] = own[:, block(me)]

    if s > 1:
        def across():
            pl.semaphore_wait(cross.at[x], cores)
            for x_at in range(xs):
                lower(x >= x_at, x_at, lambda path, distance: push_square(path, 1))
                when(
                    x >= x_at,
                    lambda: chip(lambda path: push_square(path, 1), slab, x_at),
                )
        when(first_shard, across)

    for x_at in range(xs):
        def same_chip():
            wait_for(ready.at[x_at], cores - 1 - core)
            for core_at in range(1, cores):
                def give():
                    push_square(at(slab, x_at, core_at))
                    push_piece(at(slab, x_at, core_at))
                when(core_at > core, give)

        def next_chip():
            pl.semaphore_wait(ready.at[x_at], cores)
            lower(True, x_at, lambda path, distance: push_square(path))
            chip(push_square, slab, x_at)
            if s > 1:
                def over():
                    lower(True, x_at, lambda path, distance: push_square(path, 0))
                    chip(lambda path: push_square(path, 0), slab, x_at)
                when(last_shard, over)

            lower(True, x_at, lambda path, distance: push_piece(path))
            lower(
                True,
                x_at,
                lambda path, distance: send_moment(path, distance) if distance in (1,) else None,
            )
            chip(push_piece, slab, x_at)

        when(x_at == x, same_chip)
        when(x_at > x, next_chip)

    def push_above(distance):
        def go():
            def give(x_at):
                chip(push_square, slab + distance, x_at)
                if s > 1:
                    when(
                        last_shard,
                        lambda: chip(lambda path: push_square(path, 0), slab + distance, x_at),
                    )
                chip(push_piece, slab + distance, x_at)

            for x_at in range(xs):
                def known():
                    pl.semaphore_wait(ready.at[distance * xs + x_at], cores)
                    give(x_at)
                when(x_at >= x, known)
                for low in range(x_at):
                    when(x_at == x, lambda: give(low))
        when(slab + distance < slabs, go)

    def cross_above(distance):
        def go():
            def give(x_at):
                chip(lambda path: push_square(path, 1), slab + distance, x_at)

            pl.semaphore_wait(cross.at[xs - 1 + distance], (xs - x) * cores)
            for x_at in range(xs):
                give(x_at)
        when((slab + distance < slabs) & first_shard, go)

    if slabs > 1:
        push_above(1)
    if s > 1:
        for x_at in range(1, xs):
            def rest():
                pl.semaphore_wait(cross.at[x_at], cores)
                lower(True, x_at, lambda path, distance: push_square(path, 1))
                chip(lambda path: push_square(path, 1), slab, x_at)
            when((x_at > x) & first_shard, rest)

    if slabs > 2:
        push_above(2)
    if s > 1 and slabs > 1:
        cross_above(1)
    if slabs > 3:
        push_above(3)
    if s > 1 and slabs > 2:
        cross_above(2)
    if s > 1 and slabs > 3:
        cross_above(3)

    for x_at in range(xs):
        lower(True, x_at, lambda path, distance: send_moment(path, distance) if distance in (3,) else None)

    def step_of(clipped, previous):
        moved = momentum_rate * previous + clipped
        return (outer_rate * (clipped + momentum_rate * moved)).astype(jnp.bfloat16)

    def collect(source, count, answer):
        base = source * size
        arrived(count * piece_rows + count * s + (size - count) * (s - 1), came.at[source])
        both = squares[pl.ds(base * s, size * s)].reshape(size, s, 1, LANES)
        norm_squares = jnp.sum(both, axis=1)
        shrink[pl.ds(base, size)] = jnp.minimum(1.0, limit / jnp.sqrt(norm_squares + 1e-06))

        def reply():
            for b in range(size):
                module = module_ref[base + b]
                factor = shrink[base + b]
                for low in range(0, columns, LANES):
                    lanes = pl.ds(low, LANES)
                    clipped = pieces[base + b, :, lanes].astype(jnp.float32) * factor
                    steps[base + b, :, lanes] = step_of(clipped, momentum[module, :, lanes])
            for b in range(size):
                when(base + b != me, lambda: push_step(base + b))
        when(answer, reply)

    collect(slab, size - 1, True)
    for x_at in range(xs):
        lower(True, x_at, lambda path, distance: send_moment(path, distance) if distance in (2,) else None)

    update[0, :, block(me)] = steps[me]
    for distance in range(1, slabs):
        answer = opposite(far(distance, slab - distance))
        when(
            slab >= distance,
            lambda: collect(slab - distance, size, answer),
        )
    for distance in range(1, slabs):
        when(
            slab + distance < slabs,
            lambda: collect(slab + distance, size, True),
        )

    source = [0 for _ in range(modules)]
    for path in range(n):
        for module in range(modules):
            source[module] = jnp.where(module_ref[path] == module, path, source[module])
    for module in range(modules):
        factor = shrink[source[module]]
        for low in range(0, columns, LANES):
            lanes = pl.ds(low, LANES)
            clipped = pieces[source[module], :, lanes].astype(jnp.float32) * factor
            new[module, :, lanes] = momentum_rate * momentum[module, :, lanes] + clipped

    def finish(at_slab):
        owners = [z for z in range(at_slab + 1, slabs) if far(z - at_slab, at_slab)]
        arrived(len(owners) * size * moment_rows, moment_came)
        factor = shrink[me]
        for owner in [z * size + b for z in owners for b in range(size)]:
            for low in range(0, columns, LANES):
                lanes = pl.ds(owner * columns + low, LANES)
                clipped = own[:, lanes].astype(jnp.float32) * factor
                update[0, :, lanes] = step_of(clipped, moments[owner, :, pl.ds(low, LANES)])
        told = [z for z in range(at_slab) if far(at_slab - z, z)]
        sent = (n - 1) * piece_rows + n * s - 1 + len(told) * size * moment_rows
        sent += ((slabs - len(told)) * size - 1) * piece_rows
        arrived(sent, left)
        arrived(((slabs - len(owners)) * size - 1) * piece_rows, step_came)

    for at_slab in range(slabs):
        when(slab == at_slab, lambda: finish(at_slab))


def write(update, new, update_ref, new_ref, sem):
    copies = [
        pltpu.make_async_copy(update, update_ref, sem.at[0]),
        pltpu.make_async_copy(new, new_ref, sem.at[1]),
    ]
    for copy in copies:
        copy.start()
    for copy in copies:
        copy.wait()


def direct(n, s, deltas, momentum, path_module):
    modules, rows, columns = momentum.shape
    width = deltas.shape[2]
    _, xs, slabs = grid_of(n)
    piece_rows, moment_rows = tally_rows(rows, columns)
    dma = pltpu.SemaphoreType.DMA
    regular = pltpu.SemaphoreType.REGULAR
    anywhere = pl.BlockSpec(memory_space=pl.ANY)
    in_vmem = pl.BlockSpec(memory_space=pltpu.VMEM)
    held = pl.pallas_call(
        functools.partial(kernel, n, s),
        out_shape=(
            pltpu.VMEM(deltas.shape, jnp.bfloat16),
            pltpu.VMEM(momentum.shape, jnp.float32),
        ),
        in_specs=[anywhere, anywhere, anywhere],
        out_specs=(in_vmem, in_vmem),
        scratch_shapes=[
            pltpu.SMEM(path_module.shape, jnp.int32),
            pltpu.VMEM((rows, width), jnp.bfloat16),
            pltpu.VMEM((modules, rows, columns), jnp.float32),
            pltpu.VMEM((n, rows, columns), jnp.float32),
            pltpu.VMEM((n, rows, columns), jnp.bfloat16),
            pltpu.VMEM((n, rows, columns), jnp.float32),
            pltpu.VMEM((n, rows, columns), jnp.bfloat16),
            pltpu.VMEM((1, LANES), jnp.float32),
            pltpu.VMEM((n * s, 1, LANES), jnp.float32),
            pltpu.VMEM((n, 1, LANES), jnp.float32),
            pltpu.VMEM((n * (2 * piece_rows + moment_rows + s), 1, LANES), jnp.float32),
            dma((3,)),
            regular((slabs * xs,)),
            regular((xs + slabs - 1,)),
            dma,
            dma((slabs,)),
            dma,
            dma,
        ],
        compiler_params=pltpu.CompilerParams(collective_id=0, has_side_effects=True),
    )(deltas, momentum, path_module)
    return pl.pallas_call(
        write,
        out_shape=(
            jax.ShapeDtypeStruct(deltas.shape, jnp.bfloat16),
            jax.ShapeDtypeStruct(momentum.shape, jnp.float32),
        ),
        in_specs=[in_vmem, in_vmem],
        out_specs=(anywhere, anywhere),
        scratch_shapes=[dma((2,))],
    )(*[pltpu.with_memory_space_constraint(x, pltpu.VMEM) for x in held])


def by_collectives(s, deltas, momentum, path_module):
    modules = momentum.shape[0]
    rows, width = deltas.shape[1:]
    onehot = path_module[:, None] == jnp.arange(modules, dtype=jnp.int32)[None, :]
    counts = jnp.sum(onehot.astype(jnp.float32), axis=0)
    pieces = lax.all_to_all(deltas, "path", split_axis=2, concat_axis=0, tiled=True)
    totals = jnp.einsum(
        "pm,prc->mrc", onehot.astype(jnp.bfloat16), pieces, preferred_element_type=jnp.float32
    )
    outer_grad = totals / counts[:, None, None]
    local_squares = jnp.sum(outer_grad * outer_grad, axis=(1, 2))
    norm_squares = lax.psum(local_squares, ("path", "shard"))
    limit = clip_ratio * math.sqrt(rows * s * width)
    shrink = jnp.minimum(1.0, limit / jnp.sqrt(norm_squares + 1e-06))
    clipped = outer_grad * shrink[:, None, None]
    new_momentum = momentum_rate * momentum + clipped
    outer_step = (outer_rate * (clipped + momentum_rate * new_momentum)).astype(jnp.bfloat16)
    chosen = jnp.take(outer_step, path_module, axis=0)
    path_update = lax.all_to_all(chosen, "path", split_axis=0, concat_axis=2, tiled=True)
    return (path_update, new_momentum)


def local(n, s, deltas, momentum, path_module):
    modules, rows, columns = momentum.shape
    aligned = columns % LANES == 0 and rows % 16 == 0
    one_path_each = path_module.shape[0] == modules == n
    if aligned and one_path_each and n > 1 and s <= 2:
        return direct(n, s, deltas, momentum, path_module)
    return by_collectives(s, deltas, momentum, path_module)


def solution(mesh):
    return jax.shard_map(
        functools.partial(local, mesh.shape["path"], mesh.shape["shard"]),
        mesh=mesh,
        in_specs=(P("path", "shard", None), P(None, "shard", "path"), P()),
        out_specs=(P("path", "shard", None), P(None, "shard", "path")),
        check_vma=False,
    )
```

```python
import functools
import math

import jax
import jax.numpy as jnp
from jax import lax
from jax.experimental import pallas as pl
from jax.experimental.pallas import tpu as pltpu
from jax.sharding import PartitionSpec as P

outer_rate = 0.7
momentum_rate = 0.9
clip_ratio = 2.0
LANES = 128
MESH = pl.DeviceIdType.MESH


REACH = 2
REACH_FIRST = 1


def grid_of(n):
    cores = 2 if n % 2 == 0 else 1
    xs = 2 if n % 4 == 0 else 1
    return cores, xs, n // (cores * xs)


def when(condition, act):
    if condition is True:
        act()
    elif condition is not False:
        pl.when(condition)(act)


def tally_rows(rows, columns):
    return rows * columns * 2 // (LANES * 4), rows * columns * 4 // (LANES * 4)


def opposite(condition):
    return not condition if isinstance(condition, bool) else jnp.logical_not(condition)


def kernel(
    n,
    s,
    deltas_ref,
    momentum_ref,
    path_module_ref,
    update,
    new,
    module_ref,
    own,
    momentum,
    chosen,
    pieces,
    moments,
    steps,
    mine,
    squares,
    shrink,
    tally,
    load_sem,
    ready,
    cross,
    left,
    came,
    moment_came,
    step_came,
):
    me, my_shard = lax.axis_index("path"), lax.axis_index("shard")
    modules, rows, columns = momentum.shape
    width = own.shape[1]
    cores, xs, slabs = grid_of(n)
    size = cores * xs
    core = lax.rem(me, cores)
    x = lax.rem(lax.div(me, cores), xs)
    slab = lax.div(me, size)
    limit = clip_ratio * math.sqrt(rows * s * width)
    piece_rows, moment_rows = tally_rows(rows, columns)
    first_shard, last_shard = my_shard == 0, my_shard == 1

    def arrived(count, sem):
        if count > 0:
            part = tally.at[pl.ds(0, count)]
            pltpu.make_async_copy(part, part, sem).wait()

    def signal(sem, path, shard=my_shard):
        pl.semaphore_signal(
            sem, inc=1, device_id={"path": path, "shard": shard}, device_id_type=MESH
        )

    def wait_for(sem, signals):
        when(signals > 0, lambda: pl.semaphore_wait(sem, signals))

    def block(index):
        return pl.ds(pl.multiple_of(index * columns, columns), columns)

    def send(source, target, recv_sem, path, shard=my_shard):
        pltpu.make_async_remote_copy(
            src_ref=source,
            dst_ref=target,
            send_sem=left,
            recv_sem=recv_sem,
            device_id={"path": path, "shard": shard},
            device_id_type=MESH,
        ).start()

    def push_piece(path):
        send(own.at[:, block(path)], pieces.at[me], came.at[slab], path)

    def push_moment(path, distance):
        send(chosen.at[path], moments.at[me], moment_came, path)

    def push_square(path, shard=my_shard):
        send(mine, squares.at[me * s + my_shard], came.at[slab], path, shard)

    def push_step(path):
        send(steps.at[path], update.at[0, :, block(me)], step_came, path)

    def at(z, x_at, core_at):
        return z * size + x_at * cores + core_at

    def far(distance, path_slab):
        if distance >= REACH:
            return True
        if distance >= REACH_FIRST:
            return path_slab == 0
        return False

    def chip(act, z, x_at):
        for core_at in range(cores):
            act(at(z, x_at, core_at))

    def lower(condition, x_at, act):
        for distance in range(slabs - 1, 0, -1):
            def each():
                for core_at in range(cores):
                    act(at(slab - distance, x_at, core_at), distance)
            when((slab >= distance) & condition, each)

    def beside(act):
        for x_at in range(xs):
            for core_at in range(cores):
                behind = (x > x_at) | ((x == x_at) & (core > core_at))
                when(behind, lambda: act(at(slab, x_at, core_at)))

    def send_moment(path, distance):
        when(far(distance, slab - distance), lambda: push_moment(path, distance))

    load_own = pltpu.make_async_copy(deltas_ref.at[0], own, load_sem.at[1])
    load_module = pltpu.make_async_copy(path_module_ref, module_ref, load_sem.at[0])
    load_momentum = pltpu.make_async_copy(momentum_ref, momentum, load_sem.at[2])
    load_own.start()
    load_module.start()
    load_momentum.start()

    barrier = pltpu.get_barrier_semaphore()
    for distance in range(slabs):
        for x_at in range(xs):
            inside = slab + distance < slabs
            if distance > 0:
                when(
                    inside & (x_at >= x),
                    lambda: chip(lambda path: signal(barrier, path), slab + distance, x_at),
                )
            else:
                for core_at in range(cores):
                    ahead = (x_at > x) | ((x_at == x) & (core_at > core))
                    when(ahead, lambda: signal(barrier, at(slab, x_at, core_at)))
            if s > 1:
                when(
                    inside & (x_at >= x) & first_shard,
                    lambda: chip(lambda path: signal(barrier, path, 1), slab + distance, x_at),
                )

    before = (slab * (x + 1) + x) * cores + core
    wait_for(barrier, before + my_shard * (slab + 1) * (x + 1) * cores)
    for x_at in range(xs):
        lower(
            x >= x_at, x_at, lambda path, distance: signal(ready.at[distance * xs + x], path)
        )
    beside(lambda path: signal(ready.at[x], path))
    if s > 1:
        for x_at in range(xs):
            lower(
                last_shard & (x >= x_at),
                x_at,
                lambda path, distance: signal(cross.at[xs - 1 + distance], path, 0),
            )
            when(
                last_shard & (x >= x_at),
                lambda: chip(lambda path: signal(cross.at[x], path, 0), slab, x_at),
            )

    load_own.wait()
    parts = []
    for low in range(0, width, LANES):
        held = own[:, low : low + LANES].astype(jnp.float32)
        parts.append(held * held)
    while len(parts) > 1:
        odd = parts[len(parts) // 2 * 2 :]
        parts = [a + b for a, b in zip(parts[0::2], parts[1::2])] + odd
    by_lane = jnp.sum(parts[0], axis=0, keepdims=True)
    mine[...] = jnp.broadcast_to(jnp.sum(by_lane, axis=1, keepdims=True), mine.shape)
    for x_at in range(xs):
        lower(x >= x_at, x_at, lambda path, distance: push_square(path))
        if s > 1:
            lower(
                last_shard & (x >= x_at), x_at, lambda path, distance: push_square(path, 0)
            )
            when(
                last_shard & (x >= x_at),
                lambda: chip(lambda path: push_square(path, 0), slab, x_at),
            )
    beside(push_square)
    for x_at in reversed(range(xs)):
        lower(x >= x_at, x_at, lambda path, distance: push_piece(path))
    beside(push_piece)
    squares[me * s + my_shard] = mine[...]

    load_module.wait()
    load_momentum.wait()
    for distance in range(1, slabs):
        def choose():
            for b in range(size):
                path = (slab - distance) * size + b
                chosen[path] = momentum[module_ref[path]]
        if far(distance, slab - distance) is not False:
            when((slab >= distance) & far(distance, slab - distance), choose)
    for x_at in range(xs):
        lower(
            x >= x_at,
            x_at,
            lambda path, distance: send_moment(path, distance) if distance in (1,) else None,
        )
    pieces[me] = own[:, block(me)]

    if s > 1:
        def across():
            pl.semaphore_wait(cross.at[x], cores)
            for x_at in range(xs):
                lower(x >= x_at, x_at, lambda path, distance: push_square(path, 1))
                when(
                    x >= x_at,
                    lambda: chip(lambda path: push_square(path, 1), slab, x_at),
                )
        when(first_shard, across)

    for x_at in range(xs):
        def same_chip():
            wait_for(ready.at[x_at], cores - 1 - core)
            for core_at in range(1, cores):
                def give():
                    push_square(at(slab, x_at, core_at))
                    push_piece(at(slab, x_at, core_at))
                when(core_at > core, give)

        def next_chip():
            pl.semaphore_wait(ready.at[x_at], cores)
            lower(True, x_at, lambda path, distance: push_square(path))
            chip(push_square, slab, x_at)
            if s > 1:
                def over():
                    lower(True, x_at, lambda path, distance: push_square(path, 0))
                    chip(lambda path: push_square(path, 0), slab, x_at)
                when(last_shard, over)

            lower(True, x_at, lambda path, distance: push_piece(path))
            lower(
                True,
                x_at,
                lambda path, distance: send_moment(path, distance) if distance in (1,) else None,
            )
            chip(push_piece, slab, x_at)

        when(x_at == x, same_chip)
        when(x_at > x, next_chip)

    def push_above(distance):
        def go():
            def give(x_at):
                chip(push_square, slab + distance, x_at)
                if s > 1:
                    when(
                        last_shard,
                        lambda: chip(lambda path: push_square(path, 0), slab + distance, x_at),
                    )
                chip(push_piece, slab + distance, x_at)

            for x_at in range(xs):
                def known():
                    pl.semaphore_wait(ready.at[distance * xs + x_at], cores)
                    give(x_at)
                when(x_at >= x, known)
                for low in range(x_at):
                    when(x_at == x, lambda: give(low))
        when(slab + distance < slabs, go)

    def cross_above(distance):
        def go():
            def give(x_at):
                chip(lambda path: push_square(path, 1), slab + distance, x_at)

            pl.semaphore_wait(cross.at[xs - 1 + distance], (xs - x) * cores)
            for x_at in range(xs):
                give(x_at)
        when((slab + distance < slabs) & first_shard, go)

    if slabs > 1:
        push_above(1)
    if s > 1:
        for x_at in range(1, xs):
            def rest():
                pl.semaphore_wait(cross.at[x_at], cores)
                lower(True, x_at, lambda path, distance: push_square(path, 1))
                chip(lambda path: push_square(path, 1), slab, x_at)
            when((x_at > x) & first_shard, rest)

    if slabs > 2:
        push_above(2)
    if s > 1 and slabs > 1:
        cross_above(1)
    if slabs > 3:
        push_above(3)
    if s > 1 and slabs > 2:
        cross_above(2)
    if s > 1 and slabs > 3:
        cross_above(3)

    for x_at in range(xs):
        lower(True, x_at, lambda path, distance: send_moment(path, distance) if distance in (3,) else None)

    def step_of(clipped, previous):
        moved = momentum_rate * previous + clipped
        return (outer_rate * (clipped + momentum_rate * moved)).astype(jnp.bfloat16)

    def collect(source, count, answer):
        base = source * size
        arrived(count * piece_rows + count * s + (size - count) * (s - 1), came.at[source])
        both = squares[pl.ds(base * s, size * s)].reshape(size, s, 1, LANES)
        norm_squares = jnp.sum(both, axis=1)
        shrink[pl.ds(base, size)] = jnp.minimum(1.0, limit / jnp.sqrt(norm_squares + 1e-06))

        def reply():
            for b in range(size):
                module = module_ref[base + b]
                factor = shrink[base + b]
                for low in range(0, columns, LANES):
                    lanes = pl.ds(low, LANES)
                    clipped = pieces[base + b, :, lanes].astype(jnp.float32) * factor
                    steps[base + b, :, lanes] = step_of(clipped, momentum[module, :, lanes])
            for b in range(size):
                when(base + b != me, lambda: push_step(base + b))
        when(answer, reply)

    collect(slab, size - 1, True)
    for x_at in range(xs):
        lower(True, x_at, lambda path, distance: send_moment(path, distance) if distance in (2,) else None)

    update[0, :, block(me)] = steps[me]
    for distance in range(1, slabs):
        answer = opposite(far(distance, slab - distance))
        when(
            slab >= distance,
            lambda: collect(slab - distance, size, answer),
        )
    for distance in range(1, slabs):
        when(
            slab + distance < slabs,
            lambda: collect(slab + distance, size, True),
        )

    source = [0 for _ in range(modules)]
    for path in range(n):
        for module in range(modules):
            source[module] = jnp.where(module_ref[path] == module, path, source[module])
    for module in range(modules):
        factor = shrink[source[module]]
        for low in range(0, columns, LANES):
            lanes = pl.ds(low, LANES)
            clipped = pieces[source[module], :, lanes].astype(jnp.float32) * factor
            new[module, :, lanes] = momentum_rate * momentum[module, :, lanes] + clipped

    def finish(at_slab):
        owners = [z for z in range(at_slab + 1, slabs) if far(z - at_slab, at_slab)]
        arrived(len(owners) * size * moment_rows, moment_came)
        factor = shrink[me]
        for owner in [z * size + b for z in owners for b in range(size)]:
            for low in range(0, columns, LANES):
                lanes = pl.ds(owner * columns + low, LANES)
                clipped = own[:, lanes].astype(jnp.float32) * factor
                update[0, :, lanes] = step_of(clipped, moments[owner, :, pl.ds(low, LANES)])
        told = [z for z in range(at_slab) if far(at_slab - z, z)]
        sent = (n - 1) * piece_rows + n * s - 1 + len(told) * size * moment_rows
        sent += ((slabs - len(told)) * size - 1) * piece_rows
        arrived(sent, left)
        arrived(((slabs - len(owners)) * size - 1) * piece_rows, step_came)

    for at_slab in range(slabs):
        when(slab == at_slab, lambda: finish(at_slab))


def write(update, new, update_ref, new_ref, sem):
    copies = [
        pltpu.make_async_copy(update, update_ref, sem.at[0]),
        pltpu.make_async_copy(new, new_ref, sem.at[1]),
    ]
    for copy in copies:
        copy.start()
    for copy in copies:
        copy.wait()


def direct(n, s, deltas, momentum, path_module):
    modules, rows, columns = momentum.shape
    width = deltas.shape[2]
    _, xs, slabs = grid_of(n)
    piece_rows, moment_rows = tally_rows(rows, columns)
    dma = pltpu.SemaphoreType.DMA
    regular = pltpu.SemaphoreType.REGULAR
    anywhere = pl.BlockSpec(memory_space=pl.ANY)
    in_vmem = pl.BlockSpec(memory_space=pltpu.VMEM)
    held = pl.pallas_call(
        functools.partial(kernel, n, s),
        out_shape=(
            pltpu.VMEM(deltas.shape, jnp.bfloat16),
            pltpu.VMEM(momentum.shape, jnp.float32),
        ),
        in_specs=[anywhere, anywhere, anywhere],
        out_specs=(in_vmem, in_vmem),
        scratch_shapes=[
            pltpu.SMEM(path_module.shape, jnp.int32),
            pltpu.VMEM((rows, width), jnp.bfloat16),
            pltpu.VMEM((modules, rows, columns), jnp.float32),
            pltpu.VMEM((n, rows, columns), jnp.float32),
            pltpu.VMEM((n, rows, columns), jnp.bfloat16),
            pltpu.VMEM((n, rows, columns), jnp.float32),
            pltpu.VMEM((n, rows, columns), jnp.bfloat16),
            pltpu.VMEM((1, LANES), jnp.float32),
            pltpu.VMEM((n * s, 1, LANES), jnp.float32),
            pltpu.VMEM((n, 1, LANES), jnp.float32),
            pltpu.VMEM((n * (2 * piece_rows + moment_rows + s), 1, LANES), jnp.float32),
            dma((3,)),
            regular((slabs * xs,)),
            regular((xs + slabs - 1,)),
            dma,
            dma((slabs,)),
            dma,
            dma,
        ],
        compiler_params=pltpu.CompilerParams(collective_id=0, has_side_effects=True),
    )(deltas, momentum, path_module)
    return pl.pallas_call(
        write,
        out_shape=(
            jax.ShapeDtypeStruct(deltas.shape, jnp.bfloat16),
            jax.ShapeDtypeStruct(momentum.shape, jnp.float32),
        ),
        in_specs=[in_vmem, in_vmem],
        out_specs=(anywhere, anywhere),
        scratch_shapes=[dma((2,))],
    )(*[pltpu.with_memory_space_constraint(x, pltpu.VMEM) for x in held])


def by_collectives(s, deltas, momentum, path_module):
    modules = momentum.shape[0]
    rows, width = deltas.shape[1:]
    onehot = path_module[:, None] == jnp.arange(modules, dtype=jnp.int32)[None, :]
    counts = jnp.sum(onehot.astype(jnp.float32), axis=0)
    pieces = lax.all_to_all(deltas, "path", split_axis=2, concat_axis=0, tiled=True)
    totals = jnp.einsum(
        "pm,prc->mrc", onehot.astype(jnp.bfloat16), pieces, preferred_element_type=jnp.float32
    )
    outer_grad = totals / counts[:, None, None]
    local_squares = jnp.sum(outer_grad * outer_grad, axis=(1, 2))
    norm_squares = lax.psum(local_squares, ("path", "shard"))
    limit = clip_ratio * math.sqrt(rows * s * width)
    shrink = jnp.minimum(1.0, limit / jnp.sqrt(norm_squares + 1e-06))
    clipped = outer_grad * shrink[:, None, None]
    new_momentum = momentum_rate * momentum + clipped
    outer_step = (outer_rate * (clipped + momentum_rate * new_momentum)).astype(jnp.bfloat16)
    chosen = jnp.take(outer_step, path_module, axis=0)
    path_update = lax.all_to_all(chosen, "path", split_axis=0, concat_axis=2, tiled=True)
    return (path_update, new_momentum)


def local(n, s, deltas, momentum, path_module):
    modules, rows, columns = momentum.shape
    aligned = columns % LANES == 0 and rows % 16 == 0
    one_path_each = path_module.shape[0] == modules == n
    if aligned and one_path_each and n > 1 and s <= 2:
        return direct(n, s, deltas, momentum, path_module)
    return by_collectives(s, deltas, momentum, path_module)


def solution(mesh):
    return jax.shard_map(
        functools.partial(local, mesh.shape["path"], mesh.shape["shard"]),
        mesh=mesh,
        in_specs=(P("path", "shard", None), P(None, "shard", "path"), P()),
        out_specs=(P("path", "shard", None), P(None, "shard", "path")),
        check_vma=False,
    )
```

```python
import functools
import math

import jax
import jax.numpy as jnp
from jax import lax
from jax.experimental import pallas as pl
from jax.experimental.pallas import tpu as pltpu
from jax.sharding import PartitionSpec as P

outer_rate = 0.7
momentum_rate = 0.9
clip_ratio = 2.0
LANES = 128
MESH = pl.DeviceIdType.MESH


REACH = 2
REACH_FIRST = 1


def grid_of(n):
    cores = 2 if n % 2 == 0 else 1
    xs = 2 if n % 4 == 0 else 1
    return cores, xs, n // (cores * xs)


def when(condition, act):
    if condition is True:
        act()
    elif condition is not False:
        pl.when(condition)(act)


def tally_rows(rows, columns):
    return rows * columns * 2 // (LANES * 4), rows * columns * 4 // (LANES * 4)


def opposite(condition):
    return not condition if isinstance(condition, bool) else jnp.logical_not(condition)


def kernel(
    n,
    s,
    deltas_ref,
    momentum_ref,
    path_module_ref,
    update,
    new,
    module_ref,
    own,
    momentum,
    chosen,
    pieces,
    moments,
    steps,
    mine,
    squares,
    shrink,
    tally,
    load_sem,
    ready,
    cross,
    left,
    came,
    moment_came,
    step_came,
):
    me, my_shard = lax.axis_index("path"), lax.axis_index("shard")
    modules, rows, columns = momentum.shape
    width = own.shape[1]
    cores, xs, slabs = grid_of(n)
    size = cores * xs
    core = lax.rem(me, cores)
    x = lax.rem(lax.div(me, cores), xs)
    slab = lax.div(me, size)
    limit = clip_ratio * math.sqrt(rows * s * width)
    piece_rows, moment_rows = tally_rows(rows, columns)
    first_shard, last_shard = my_shard == 0, my_shard == 1

    def arrived(count, sem):
        if count > 0:
            part = tally.at[pl.ds(0, count)]
            pltpu.make_async_copy(part, part, sem).wait()

    def signal(sem, path, shard=my_shard):
        pl.semaphore_signal(
            sem, inc=1, device_id={"path": path, "shard": shard}, device_id_type=MESH
        )

    def wait_for(sem, signals):
        when(signals > 0, lambda: pl.semaphore_wait(sem, signals))

    def block(index):
        return pl.ds(pl.multiple_of(index * columns, columns), columns)

    def send(source, target, recv_sem, path, shard=my_shard):
        pltpu.make_async_remote_copy(
            src_ref=source,
            dst_ref=target,
            send_sem=left,
            recv_sem=recv_sem,
            device_id={"path": path, "shard": shard},
            device_id_type=MESH,
        ).start()

    def push_piece(path):
        send(own.at[:, block(path)], pieces.at[me], came.at[slab], path)

    def push_moment(path, distance):
        send(chosen.at[path], moments.at[me], moment_came, path)

    def push_square(path, shard=my_shard):
        send(mine, squares.at[me * s + my_shard], came.at[slab], path, shard)

    def push_step(path):
        send(steps.at[path], update.at[0, :, block(me)], step_came, path)

    def at(z, x_at, core_at):
        return z * size + x_at * cores + core_at

    def far(distance, path_slab):
        if distance >= REACH:
            return True
        if distance >= REACH_FIRST:
            return path_slab == 0
        return False

    def chip(act, z, x_at):
        for core_at in range(cores):
            act(at(z, x_at, core_at))

    def lower(condition, x_at, act):
        for distance in range(slabs - 1, 0, -1):
            def each():
                for core_at in range(cores):
                    act(at(slab - distance, x_at, core_at), distance)
            when((slab >= distance) & condition, each)

    def beside(act):
        for x_at in range(xs):
            for core_at in range(cores):
                behind = (x > x_at) | ((x == x_at) & (core > core_at))
                when(behind, lambda: act(at(slab, x_at, core_at)))

    def send_moment(path, distance):
        when(far(distance, slab - distance), lambda: push_moment(path, distance))

    load_own = pltpu.make_async_copy(deltas_ref.at[0], own, load_sem.at[1])
    load_module = pltpu.make_async_copy(path_module_ref, module_ref, load_sem.at[0])
    load_momentum = pltpu.make_async_copy(momentum_ref, momentum, load_sem.at[2])
    load_own.start()
    load_module.start()
    load_momentum.start()

    barrier = pltpu.get_barrier_semaphore()
    for distance in range(slabs):
        for x_at in range(xs):
            inside = slab + distance < slabs
            if distance > 0:
                when(
                    inside & (x_at >= x),
                    lambda: chip(lambda path: signal(barrier, path), slab + distance, x_at),
                )
            else:
                for core_at in range(cores):
                    ahead = (x_at > x) | ((x_at == x) & (core_at > core))
                    when(ahead, lambda: signal(barrier, at(slab, x_at, core_at)))
            if s > 1:
                when(
                    inside & (x_at >= x) & first_shard,
                    lambda: chip(lambda path: signal(barrier, path, 1), slab + distance, x_at),
                )

    before = (slab * (x + 1) + x) * cores + core
    wait_for(barrier, before + my_shard * (slab + 1) * (x + 1) * cores)
    if s > 1:
        for x_at in range(xs):
            lower(
                last_shard & (x >= x_at),
                x_at,
                lambda path, distance: signal(cross.at[xs - 1 + distance], path, 0),
            )
            when(
                last_shard & (x >= x_at),
                lambda: chip(lambda path: signal(cross.at[x], path, 0), slab, x_at),
            )
    for x_at in range(xs):
        lower(
            x >= x_at, x_at, lambda path, distance: signal(ready.at[distance * xs + x], path)
        )
    beside(lambda path: signal(ready.at[x], path))

    load_own.wait()
    parts = []
    for low in range(0, width, LANES):
        held = own[:, low : low + LANES].astype(jnp.float32)
        parts.append(held * held)
    while len(parts) > 1:
        odd = parts[len(parts) // 2 * 2 :]
        parts = [a + b for a, b in zip(parts[0::2], parts[1::2])] + odd
    by_lane = jnp.sum(parts[0], axis=0, keepdims=True)
    mine[...] = jnp.broadcast_to(jnp.sum(by_lane, axis=1, keepdims=True), mine.shape)
    for x_at in range(xs):
        lower(x >= x_at, x_at, lambda path, distance: push_square(path))
        if s > 1:
            lower(
                last_shard & (x >= x_at), x_at, lambda path, distance: push_square(path, 0)
            )
            when(
                last_shard & (x >= x_at),
                lambda: chip(lambda path: push_square(path, 0), slab, x_at),
            )
    beside(push_square)
    for x_at in reversed(range(xs)):
        lower(x >= x_at, x_at, lambda path, distance: push_piece(path))
    beside(push_piece)
    squares[me * s + my_shard] = mine[...]

    load_module.wait()
    load_momentum.wait()
    for distance in range(1, slabs):
        def choose():
            for b in range(size):
                path = (slab - distance) * size + b
                chosen[path] = momentum[module_ref[path]]
        if far(distance, slab - distance) is not False:
            when((slab >= distance) & far(distance, slab - distance), choose)
    for x_at in range(xs):
        lower(
            x >= x_at,
            x_at,
            lambda path, distance: send_moment(path, distance) if distance in (1,) else None,
        )
    pieces[me] = own[:, block(me)]

    if s > 1:
        def across():
            pl.semaphore_wait(cross.at[x], cores)
            for x_at in range(xs):
                lower(x >= x_at, x_at, lambda path, distance: push_square(path, 1))
                when(
                    x >= x_at,
                    lambda: chip(lambda path: push_square(path, 1), slab, x_at),
                )
        when(first_shard, across)

    for x_at in range(xs):
        def same_chip():
            wait_for(ready.at[x_at], cores - 1 - core)
            for core_at in range(1, cores):
                def give():
                    push_square(at(slab, x_at, core_at))
                    push_piece(at(slab, x_at, core_at))
                when(core_at > core, give)

        def next_chip():
            pl.semaphore_wait(ready.at[x_at], cores)
            lower(True, x_at, lambda path, distance: push_square(path))
            chip(push_square, slab, x_at)
            if s > 1:
                def over():
                    lower(True, x_at, lambda path, distance: push_square(path, 0))
                    chip(lambda path: push_square(path, 0), slab, x_at)
                when(last_shard, over)

            lower(True, x_at, lambda path, distance: push_piece(path))
            lower(
                True,
                x_at,
                lambda path, distance: send_moment(path, distance) if distance in (1,) else None,
            )
            chip(push_piece, slab, x_at)

        when(x_at == x, same_chip)
        when(x_at > x, next_chip)

    def push_above(distance):
        def go():
            def give(x_at):
                chip(push_square, slab + distance, x_at)
                if s > 1:
                    when(
                        last_shard,
                        lambda: chip(lambda path: push_square(path, 0), slab + distance, x_at),
                    )
                chip(push_piece, slab + distance, x_at)

            for x_at in range(xs):
                def known():
                    pl.semaphore_wait(ready.at[distance * xs + x_at], cores)
                    give(x_at)
                when(x_at >= x, known)
                for low in range(x_at):
                    when(x_at == x, lambda: give(low))
        when(slab + distance < slabs, go)

    def cross_above(distance):
        def go():
            def give(x_at):
                chip(lambda path: push_square(path, 1), slab + distance, x_at)

            pl.semaphore_wait(cross.at[xs - 1 + distance], (xs - x) * cores)
            for x_at in range(xs):
                give(x_at)
        when((slab + distance < slabs) & first_shard, go)

    if slabs > 1:
        push_above(1)
    if s > 1:
        for x_at in range(1, xs):
            def rest():
                pl.semaphore_wait(cross.at[x_at], cores)
                lower(True, x_at, lambda path, distance: push_square(path, 1))
                chip(lambda path: push_square(path, 1), slab, x_at)
            when((x_at > x) & first_shard, rest)

    if slabs > 2:
        push_above(2)
    if s > 1 and slabs > 1:
        cross_above(1)
    if slabs > 3:
        push_above(3)
    if s > 1 and slabs > 2:
        cross_above(2)
    if s > 1 and slabs > 3:
        cross_above(3)

    for x_at in range(xs):
        lower(True, x_at, lambda path, distance: send_moment(path, distance) if distance in (3,) else None)

    def step_of(clipped, previous):
        moved = momentum_rate * previous + clipped
        return (outer_rate * (clipped + momentum_rate * moved)).astype(jnp.bfloat16)

    def collect(source, count, answer):
        base = source * size
        arrived(count * piece_rows + count * s + (size - count) * (s - 1), came.at[source])
        both = squares[pl.ds(base * s, size * s)].reshape(size, s, 1, LANES)
        norm_squares = jnp.sum(both, axis=1)
        shrink[pl.ds(base, size)] = jnp.minimum(1.0, limit / jnp.sqrt(norm_squares + 1e-06))

        def reply():
            for b in range(size):
                module = module_ref[base + b]
                factor = shrink[base + b]
                for low in range(0, columns, LANES):
                    lanes = pl.ds(low, LANES)
                    clipped = pieces[base + b, :, lanes].astype(jnp.float32) * factor
                    steps[base + b, :, lanes] = step_of(clipped, momentum[module, :, lanes])
            for b in range(size):
                when(base + b != me, lambda: push_step(base + b))
        when(answer, reply)

    collect(slab, size - 1, True)
    for x_at in range(xs):
        lower(True, x_at, lambda path, distance: send_moment(path, distance) if distance in (2,) else None)

    update[0, :, block(me)] = steps[me]
    for distance in range(1, slabs):
        answer = opposite(far(distance, slab - distance))
        when(
            slab >= distance,
            lambda: collect(slab - distance, size, answer),
        )
    for distance in range(1, slabs):
        when(
            slab + distance < slabs,
            lambda: collect(slab + distance, size, True),
        )

    source = [0 for _ in range(modules)]
    for path in range(n):
        for module in range(modules):
            source[module] = jnp.where(module_ref[path] == module, path, source[module])
    for module in range(modules):
        factor = shrink[source[module]]
        for low in range(0, columns, LANES):
            lanes = pl.ds(low, LANES)
            clipped = pieces[source[module], :, lanes].astype(jnp.float32) * factor
            new[module, :, lanes] = momentum_rate * momentum[module, :, lanes] + clipped

    def finish(at_slab):
        owners = [z for z in range(at_slab + 1, slabs) if far(z - at_slab, at_slab)]
        arrived(len(owners) * size * moment_rows, moment_came)
        factor = shrink[me]
        for owner in [z * size + b for z in owners for b in range(size)]:
            for low in range(0, columns, LANES):
                lanes = pl.ds(owner * columns + low, LANES)
                clipped = own[:, lanes].astype(jnp.float32) * factor
                update[0, :, lanes] = step_of(clipped, moments[owner, :, pl.ds(low, LANES)])
        told = [z for z in range(at_slab) if far(at_slab - z, z)]
        sent = (n - 1) * piece_rows + n * s - 1 + len(told) * size * moment_rows
        sent += ((slabs - len(told)) * size - 1) * piece_rows
        arrived(sent, left)
        arrived(((slabs - len(owners)) * size - 1) * piece_rows, step_came)

    for at_slab in range(slabs):
        when(slab == at_slab, lambda: finish(at_slab))


def write(update, new, update_ref, new_ref, sem):
    copies = [
        pltpu.make_async_copy(update, update_ref, sem.at[0]),
        pltpu.make_async_copy(new, new_ref, sem.at[1]),
    ]
    for copy in copies:
        copy.start()
    for copy in copies:
        copy.wait()


def direct(n, s, deltas, momentum, path_module):
    modules, rows, columns = momentum.shape
    width = deltas.shape[2]
    _, xs, slabs = grid_of(n)
    piece_rows, moment_rows = tally_rows(rows, columns)
    dma = pltpu.SemaphoreType.DMA
    regular = pltpu.SemaphoreType.REGULAR
    anywhere = pl.BlockSpec(memory_space=pl.ANY)
    in_vmem = pl.BlockSpec(memory_space=pltpu.VMEM)
    held = pl.pallas_call(
        functools.partial(kernel, n, s),
        out_shape=(
            pltpu.VMEM(deltas.shape, jnp.bfloat16),
            pltpu.VMEM(momentum.shape, jnp.float32),
        ),
        in_specs=[anywhere, anywhere, anywhere],
        out_specs=(in_vmem, in_vmem),
        scratch_shapes=[
            pltpu.SMEM(path_module.shape, jnp.int32),
            pltpu.VMEM((rows, width), jnp.bfloat16),
            pltpu.VMEM((modules, rows, columns), jnp.float32),
            pltpu.VMEM((n, rows, columns), jnp.float32),
            pltpu.VMEM((n, rows, columns), jnp.bfloat16),
            pltpu.VMEM((n, rows, columns), jnp.float32),
            pltpu.VMEM((n, rows, columns), jnp.bfloat16),
            pltpu.VMEM((1, LANES), jnp.float32),
            pltpu.VMEM((n * s, 1, LANES), jnp.float32),
            pltpu.VMEM((n, 1, LANES), jnp.float32),
            pltpu.VMEM((n * (2 * piece_rows + moment_rows + s), 1, LANES), jnp.float32),
            dma((3,)),
            regular((slabs * xs,)),
            regular((xs + slabs - 1,)),
            dma,
            dma((slabs,)),
            dma,
            dma,
        ],
        compiler_params=pltpu.CompilerParams(collective_id=0, has_side_effects=True),
    )(deltas, momentum, path_module)
    return pl.pallas_call(
        write,
        out_shape=(
            jax.ShapeDtypeStruct(deltas.shape, jnp.bfloat16),
            jax.ShapeDtypeStruct(momentum.shape, jnp.float32),
        ),
        in_specs=[in_vmem, in_vmem],
        out_specs=(anywhere, anywhere),
        scratch_shapes=[dma((2,))],
    )(*[pltpu.with_memory_space_constraint(x, pltpu.VMEM) for x in held])


def by_collectives(s, deltas, momentum, path_module):
    modules = momentum.shape[0]
    rows, width = deltas.shape[1:]
    onehot = path_module[:, None] == jnp.arange(modules, dtype=jnp.int32)[None, :]
    counts = jnp.sum(onehot.astype(jnp.float32), axis=0)
    pieces = lax.all_to_all(deltas, "path", split_axis=2, concat_axis=0, tiled=True)
    totals = jnp.einsum(
        "pm,prc->mrc", onehot.astype(jnp.bfloat16), pieces, preferred_element_type=jnp.float32
    )
    outer_grad = totals / counts[:, None, None]
    local_squares = jnp.sum(outer_grad * outer_grad, axis=(1, 2))
    norm_squares = lax.psum(local_squares, ("path", "shard"))
    limit = clip_ratio * math.sqrt(rows * s * width)
    shrink = jnp.minimum(1.0, limit / jnp.sqrt(norm_squares + 1e-06))
    clipped = outer_grad * shrink[:, None, None]
    new_momentum = momentum_rate * momentum + clipped
    outer_step = (outer_rate * (clipped + momentum_rate * new_momentum)).astype(jnp.bfloat16)
    chosen = jnp.take(outer_step, path_module, axis=0)
    path_update = lax.all_to_all(chosen, "path", split_axis=0, concat_axis=2, tiled=True)
    return (path_update, new_momentum)


def local(n, s, deltas, momentum, path_module):
    modules, rows, columns = momentum.shape
    aligned = columns % LANES == 0 and rows % 16 == 0
    one_path_each = path_module.shape[0] == modules == n
    if aligned and one_path_each and n > 1 and s <= 2:
        return direct(n, s, deltas, momentum, path_module)
    return by_collectives(s, deltas, momentum, path_module)


def solution(mesh):
    return jax.shard_map(
        functools.partial(local, mesh.shape["path"], mesh.shape["shard"]),
        mesh=mesh,
        in_specs=(P("path", "shard", None), P(None, "shard", "path"), P()),
        out_specs=(P("path", "shard", None), P(None, "shard", "path")),
        check_vma=False,
    )
```
